512 devices in a mesh: acq: 16 (over z, y_lo), line: 32 (over y_hi, x, core).
Axes of the slice: x: 4, y: 8 (y_hi: 4, y_lo: 2; y = y_hi * 2 + y_lo), z: 8, core: 2. Of those that a mesh axis runs over, the one named last changes fastest.
Arguments:
- slc_stack: float32 [2, 64, 256, 2048], P(None, 'acq', 'line'), may hold values from -6 to 6
- wavenumbers: float32 [64], replicated, may hold values from -0.8 to 0.8
Outputs:
- spectrum: bfloat16 [256, 256, 2048], P(None, 'line', 'acq')
The draws below stay inside these ranges and needn't reach their ends.
All inputs are finite; a program needn't handle non-finite values.
Results may differ from the reference program's by a relative error of at most 0.001.
Values sent between devices are 32-bit elements; how exact they have to be, the bound alone decides.
No kernel may reach another device: no remote copies, remote signals or barrier semaphores. Data moves between devices by JAX's collectives and lax.ppermute only.
A program may use at most 64 MiB of HBM per device.

```python
import jax
import jax.numpy as jnp
from jax import lax

ACQS = 64
HEIGHTS = 256
LINE_DEV = 8
LINES = 256
RANGE = 2048
N_LINE = 32


def block_scale(key, dims, pieces, smallest, largest):
    gain = 1.0
    for position, parts in pieces:
        steps = jax.random.uniform(jax.random.fold_in(jax.random.fold_in(key, 6), position), (parts,), jnp.float32, smallest / len(pieces), largest / len(pieces))
        gain = gain * jnp.repeat(jnp.exp(steps), dims[position] // parts).reshape((-1,) + (1,) * (len(dims) - 1 - position))
    return gain


def noise(own_key, shape, width, most, cuts=(), held_as=jnp.bfloat16):
    array = width * jax.random.normal(own_key, shape, jnp.float32)
    if cuts:
        array = array * block_scale(own_key, shape, cuts, -0.22, 0.18)
    return jnp.clip(array, -most, most).astype(held_as)


def setup_inputs(seed: int = 0) -> dict:
    streams_of = jax.random.split(jax.random.key(seed), 3)
    slc_stack = noise(streams_of[0], (2, ACQS, LINES, RANGE), 1.0, 6.0, ((1, 16), (2, 32)), jnp.float32)
    wavenumbers = jnp.clip(jax.random.uniform(streams_of[1], (ACQS,), jnp.float32, -0.8, 0.8), -0.8, 0.8)
    return dict(slc_stack=slc_stack, wavenumbers=wavenumbers)


epsilon = 1e-6


def steering(wavenumbers, count):
    heights = jnp.arange(count, dtype=jnp.int32).astype(jnp.float32) - jnp.float32(count // 2)
    phases = wavenumbers[:, None] * heights[None, :]
    cosine_part = jnp.cos(phases).T
    sine_part = jnp.sin(phases).T
    upper = jnp.concatenate([cosine_part, sine_part], axis=1)
    lower = jnp.concatenate([-sine_part, cosine_part], axis=1)
    return jnp.concatenate([upper, lower], axis=0)


def beamform(stack_block, wavenumbers, count):
    matrix = steering(wavenumbers, count)
    channels = stack_block.shape[0] * stack_block.shape[1]
    flat = stack_block.reshape(channels, -1)
    beams = jnp.dot(matrix, flat, precision=lax.Precision.HIGHEST, preferred_element_type=jnp.float32)
    beam_power = beams[:count] * beams[:count] + beams[count:] * beams[count:]
    energy = jnp.sum(flat * flat, axis=0)
    shape = stack_block.shape[2:]
    return beam_power.reshape((count,) + shape), energy.reshape((1,) + shape)


def sum_range(field, count):
    total = field[..., 0:count]
    for offset in range(1, 7):
        total = total + field[..., offset:offset + count]
    return total


def sum_lines(field, count):
    total = field[..., 0:count, :]
    for offset in range(1, 7):
        total = total + field[..., offset:offset + count, :]
    return total


def reference(slc_stack, wavenumbers):
    padded = jnp.pad(slc_stack, ((0, 0), (0, 0), (3, 3), (3, 3)))
    range_count = slc_stack.shape[3]

    def one_block(block_index):
        first_line = (block_index * LINE_DEV).astype(jnp.int32)
        stack_block = lax.dynamic_slice_in_dim(padded, first_line, LINE_DEV + 6, 2)
        beam_power, energy = beamform(stack_block, wavenumbers, HEIGHTS)
        box_power = sum_lines(sum_range(beam_power, range_count), LINE_DEV)
        box_energy = sum_lines(sum_range(energy, range_count), LINE_DEV)
        return (box_power / (box_energy + epsilon)).astype(jnp.bfloat16)

    blocks = lax.map(one_block, jnp.arange(N_LINE, dtype=jnp.int32))
    return blocks.transpose(1, 0, 2, 3).reshape(HEIGHTS, LINE_DEV * N_LINE, range_count)
```

```python
import jax
import jax.numpy as jnp
import numpy as np
from jax import lax
from jax.experimental import pallas as pl
from jax.experimental.pallas import tpu as pltpu
from jax.sharding import PartitionSpec as P


HEIGHTS = 256
ROWS = HEIGHTS + 8
LANES = 128
epsilon = 1e-06

SLOT = {0: 0, 1: 1, 2: 2, 7: 4, 6: 5, 5: 6, 3: 7, 4: 8}
HALO = 3

PACK_VMEM = 4 << 20
OWN_VMEM = 10 << 20
BOX_VMEM = 16 << 20


def parity():
    return lax.rem(lax.axis_index("line"), 2)


def pack_kernel(x_ref, out_ref):
    blocks = x_ref.shape[0] // 64
    odd = parity()
    lane = lax.broadcasted_iota(jnp.int32, (8, LANES), 1)
    halo = [jnp.zeros((8, LANES), jnp.float32) for _ in range(blocks)]
    for m in range(8):
        line = m + odd * (7 - 2 * m)
        left = (lane >= 6 * m) & (lane < 6 * m + 3)
        right = (lane >= 6 * m + 3) & (lane < 6 * m + 6)
        for j in range(blocks):
            tile = x_ref[pl.ds(8 * j + line, 8, stride=8 * blocks), :]
            out_ref[j, SLOT[m]] = tile
            moved = pltpu.roll(tile, 3 + 6 * m, 1)
            if j + 1 < blocks:
                halo[j + 1] = jnp.where(left, moved, halo[j + 1])
            if j >= 1:
                halo[j - 1] = jnp.where(right, moved, halo[j - 1])
    for j in range(blocks):
        out_ref[j, HALO] = halo[j]


def beam_pair(first, second, steer_ref, beams_ref):
    both = jnp.concatenate([first.reshape(LANES, LANES), second.reshape(LANES, LANES)], axis=1)
    high = both.astype(jnp.bfloat16)
    low = (both - high.astype(jnp.float32)).astype(jnp.bfloat16)
    stacked = jnp.concatenate([high, low, high], axis=0)
    beams_ref[...] = jnp.dot(steer_ref[...], stacked, preferred_element_type=jnp.float32)
    re, im = beams_ref[:HEIGHTS], beams_ref[HEIGHTS:]
    power = re * re + im * im
    squares = (both * both).reshape(16, 8, 2 * LANES).sum(axis=0)
    return jnp.concatenate([power, squares], axis=0)


def own_kernel(r_ref, steer_ref, out_ref, beams_ref):
    for s in (0, 2, 4, 6, 8):
        t = min(s + 1, 8)
        both = beam_pair(r_ref[:, s], r_ref[:, t], steer_ref, beams_ref)
        out_ref[s] = both[:, :LANES]
        if t != s:
            out_ref[t] = both[:, LANES:]


def halves(field):
    high = field.astype(jnp.bfloat16)
    low = (field - high.astype(jnp.float32)).astype(jnp.bfloat16)
    return jnp.concatenate([high, low], axis=1)


def box_kernel(own_ref, o_ref, e_ref, steer_ref, mid_ref, mo_ref, me_ref, out_ref, beams_ref, side_ref, cor_ref, flat_ref):
    odd = parity()
    for k, ref in ((0, o_ref), (4, e_ref)):
        for s in (0, 2):
            both = beam_pair(ref[:, s], ref[:, s + 1], steer_ref, beams_ref)
            side_ref[k + s] = both[:, :LANES]
            side_ref[k + s + 1] = both[:, LANES:]
    cor_ref[...] = jnp.dot(halves(own_ref[HALO]), mid_ref[...], preferred_element_type=jnp.float32)
    cor_ref[:, : 3 * LANES] += jnp.dot(halves(side_ref[3]), mo_ref[...], preferred_element_type=jnp.float32)
    cor_ref[:, 5 * LANES :] += jnp.dot(halves(side_ref[4]), me_ref[...], preferred_element_type=jnp.float32)

    def rows_of(position, rows):
        if position < 0:
            return side_ref[-1 - position, rows]
        if position > 7:
            return side_ref[position - 3, rows]
        return own_ref[SLOT[position], rows]

    def boxed(m, rows, count):
        lane = lax.broadcasted_iota(jnp.int32, (count, LANES), 1)
        total = rows_of(m - 3, rows)
        for d in range(-2, 4):
            total = total + rows_of(m + d, rows)
        box = total + cor_ref[rows, m * LANES : (m + 1) * LANES]
        for d in (1, 2, 3):
            box = box + jnp.where(lane >= d, pltpu.roll(total, d, 1), 0.0)
            box = box + jnp.where(lane < LANES - d, pltpu.roll(total, LANES - d, 1), 0.0)
        return box

    for m in range(8):
        line = m + odd * (7 - 2 * m)
        energy = boxed(m, slice(HEIGHTS, ROWS), 8).sum(axis=0, keepdims=True)
        inverse = 1.0 / (energy + epsilon)
        for k in range(0, HEIGHTS, 64):
            box = boxed(m, slice(k, k + 64), 64) * inverse
            flat_ref[pl.ds(8 * k + line, 64, stride=8), :] = box
    for k in range(0, HEIGHTS, 16):
        out_ref[k : k + 16] = flat_ref[8 * k : 8 * k + 128].reshape(16, 8, LANES).astype(jnp.bfloat16)


def spread():
    column = np.array([-3, -2, -1, 128, 129, 130])
    near = np.abs(column[:, None] - np.arange(LANES)[None, :]) <= 3

    def matrix(position_of, lines, used):
        full = np.zeros((LANES, len(lines), LANES), np.float32)
        for n in used:
            for i, m in enumerate(lines):
                if abs(position_of(n) - m) <= 3:
                    full[6 * n : 6 * n + 6, i] = near
        full = full.reshape(LANES, -1)
        return jnp.asarray(np.concatenate([full, full], axis=0), jnp.bfloat16)

    mid = matrix(lambda n: n, range(8), range(8))
    mo = matrix(lambda n: -1 - n, (0, 1, 2), (0, 1, 2))
    me = matrix(lambda n: 15 - n, (5, 6, 7), (5, 6, 7))
    return mid, mo, me


def steering(wavenumbers):
    waves = jnp.broadcast_to(wavenumbers.reshape(16, 1, 4), (16, 2, 4)).reshape(LANES)
    real = (jnp.arange(LANES) // 4) % 2 == 0
    heights = jnp.arange(HEIGHTS, dtype=jnp.int32).astype(jnp.float32) - jnp.float32(HEIGHTS // 2)
    phases = heights[:, None] * waves[None, :]
    cosine, sine = jnp.cos(phases), jnp.sin(phases)
    full = jnp.concatenate([jnp.where(real, cosine, sine), jnp.where(real, -sine, cosine)], axis=0)
    high = lax.reduce_precision(full, 8, 7)
    low = (full - high).astype(jnp.bfloat16)
    high = high.astype(jnp.bfloat16)
    return jnp.concatenate([high, high, low], axis=1)


VMEM = pl.BlockSpec(memory_space=pltpu.VMEM)


def spectrum(slc_stack, wavenumbers):
    lines = lax.axis_size("line")
    outer = [pair for i in range(1, lines - 1, 2) for pair in ((i, i + 1), (i + 1, i))]
    inner = [pair for i in range(0, lines, 2) for pair in ((i, i + 1), (i + 1, i))]
    packed = pl.pallas_call(
        pack_kernel,
        out_shape=jax.ShapeDtypeStruct((16, 9, 8, LANES), jnp.float32),
        in_specs=[VMEM],
        out_specs=VMEM,
        name="pack",
        compiler_params=pltpu.CompilerParams(vmem_limit_bytes=PACK_VMEM),
        cost_estimate=pl.CostEstimate(flops=1000000, bytes_accessed=1100000, transcendentals=0),
    )(slc_stack.reshape(8, 8, -1, LANES).transpose(0, 2, 1, 3).reshape(-1, LANES))
    gathered = lax.all_to_all(packed, "acq", 0, 0, tiled=True)
    steer = steering(wavenumbers)
    mid, mo, me = spread()
    side_o = lax.ppermute(gathered[:, 0:4], "line", outer)
    side_e = lax.ppermute(gathered[:, 3:7], "line", inner)
    own = pl.pallas_call(
        own_kernel,
        out_shape=jax.ShapeDtypeStruct((9, ROWS, LANES), jnp.float32),
        in_specs=[VMEM] * 2,
        out_specs=VMEM,
        scratch_shapes=[pltpu.VMEM((2 * HEIGHTS, 2 * LANES), jnp.float32)],
        name="own",
        compiler_params=pltpu.CompilerParams(vmem_limit_bytes=OWN_VMEM),
        cost_estimate=pl.CostEstimate(flops=1000000000, bytes_accessed=2000000, transcendentals=0),
    )(gathered, steer)
    return pl.pallas_call(
        box_kernel,
        out_shape=jax.ShapeDtypeStruct((HEIGHTS, 8, LANES), jnp.bfloat16),
        in_specs=[VMEM] * 7,
        out_specs=VMEM,
        scratch_shapes=[
            pltpu.VMEM((2 * HEIGHTS, 2 * LANES), jnp.float32),
            pltpu.VMEM((8, ROWS, LANES), jnp.float32),
            pltpu.VMEM((ROWS, 8 * LANES), jnp.float32),
            pltpu.VMEM((8 * HEIGHTS, LANES), jnp.float32),
        ],
        name="box",
        compiler_params=pltpu.CompilerParams(vmem_limit_bytes=BOX_VMEM),
        cost_estimate=pl.CostEstimate(flops=1000000000, bytes_accessed=2000000, transcendentals=0),
    )(own, side_o, side_e, steer, mid, mo, me)


def solution(mesh):
    placed = (P(None, "acq", "line", None), P())
    return jax.shard_map(spectrum, mesh=mesh, in_specs=placed, out_specs=P(None, "line", "acq"), check_vma=False)
```

```python
import jax
import jax.numpy as jnp
import numpy as np
from jax import lax
from jax.experimental import pallas as pl
from jax.experimental.pallas import tpu as pltpu
from jax.sharding import PartitionSpec as P


HEIGHTS = 256
ROWS = HEIGHTS + 8
LANES = 128
epsilon = 1e-06

SLOT = {0: 0, 1: 1, 2: 2, 7: 4, 6: 5, 5: 6, 3: 7, 4: 8}
HALO = 3
FIRST = 4

PACK_VMEM = 4 << 20
OWN_VMEM = 10 << 20
BOX_VMEM = 16 << 20


def parity():
    return lax.rem(lax.axis_index("line"), 2)


def tile_of(x_ref, m, odd, j):
    blocks = x_ref.shape[0] // 64
    return x_ref[pl.ds(8 * j + m + odd * (7 - 2 * m), 8, stride=8 * blocks), :]


def pack_edge(x_ref, out_ref):
    blocks = x_ref.shape[0] // 64
    odd = parity()
    lane = lax.broadcasted_iota(jnp.int32, (8, LANES), 1)
    halo = [jnp.zeros((8, LANES), jnp.float32) for _ in range(blocks)]
    for m in range(8):
        left = (lane >= 6 * m) & (lane < 6 * m + 3)
        right = (lane >= 6 * m + 3) & (lane < 6 * m + 6)
        for j in range(blocks):
            tile = tile_of(x_ref, m, odd, j)
            if SLOT[m] < FIRST:
                out_ref[j, SLOT[m]] = tile
            moved = pltpu.roll(tile, 3 + 6 * m, 1)
            if j + 1 < blocks:
                halo[j + 1] = jnp.where(left, moved, halo[j + 1])
            if j >= 1:
                halo[j - 1] = jnp.where(right, moved, halo[j - 1])
    for j in range(blocks):
        out_ref[j, HALO] = halo[j]


def pack_rest(x_ref, steer_ref, out_ref):
    odd = parity()
    for m in range(3, 8):
        for j in range(x_ref.shape[0] // 64):
            out_ref[j, SLOT[m] - FIRST] = tile_of(x_ref, m, odd, j)


def beam_pair(first, second, steer_ref, beams_ref):
    both = jnp.concatenate([first.reshape(LANES, LANES), second.reshape(LANES, LANES)], axis=1)
    high = both.astype(jnp.bfloat16)
    low = (both - high.astype(jnp.float32)).astype(jnp.bfloat16)
    stacked = jnp.concatenate([high, low, high], axis=0)
    beams_ref[...] = jnp.dot(steer_ref[...], stacked, preferred_element_type=jnp.float32)
    re, im = beams_ref[:HEIGHTS], beams_ref[HEIGHTS:]
    power = re * re + im * im
    squares = (both * both).reshape(16, 8, 2 * LANES).sum(axis=0)
    return jnp.concatenate([power, squares], axis=0)


def own_kernel(r_ref, steer_ref, out_ref, beams_ref):
    count = r_ref.shape[1]
    for s in range(0, count, 2):
        t = min(s + 1, count - 1)
        both = beam_pair(r_ref[:, s], r_ref[:, t], steer_ref, beams_ref)
        out_ref[s] = both[:, :LANES]
        if t != s:
            out_ref[t] = both[:, LANES:]


def halves(field):
    high = field.astype(jnp.bfloat16)
    low = (field - high.astype(jnp.float32)).astype(jnp.bfloat16)
    return jnp.concatenate([high, low], axis=1)


def box_kernel(edge_ref, rest_ref, o_ref, e_ref, steer_ref, mid_ref, mo_ref, me_ref, out_ref, beams_ref, side_ref, cor_ref, flat_ref):
    odd = parity()
    for k, ref in ((0, o_ref), (4, e_ref)):
        for s in (0, 2):
            both = beam_pair(ref[:, s], ref[:, s + 1], steer_ref, beams_ref)
            side_ref[k + s] = both[:, :LANES]
            side_ref[k + s + 1] = both[:, LANES:]
    cor_ref[...] = jnp.dot(halves(edge_ref[HALO]), mid_ref[...], preferred_element_type=jnp.float32)
    cor_ref[:, : 3 * LANES] += jnp.dot(halves(side_ref[3]), mo_ref[...], preferred_element_type=jnp.float32)
    cor_ref[:, 5 * LANES :] += jnp.dot(halves(side_ref[4]), me_ref[...], preferred_element_type=jnp.float32)

    def rows_of(position, rows):
        if position < 0:
            return side_ref[-1 - position, rows]
        if position > 7:
            return side_ref[position - 3, rows]
        slot = SLOT[position]
        return edge_ref[slot, rows] if slot < FIRST else rest_ref[slot - FIRST, rows]

    def boxed(m, rows, count):
        lane = lax.broadcasted_iota(jnp.int32, (count, LANES), 1)
        total = rows_of(m - 3, rows)
        for d in range(-2, 4):
            total = total + rows_of(m + d, rows)
        box = total + cor_ref[rows, m * LANES : (m + 1) * LANES]
        for d in (1, 2, 3):
            box = box + jnp.where(lane >= d, pltpu.roll(total, d, 1), 0.0)
            box = box + jnp.where(lane < LANES - d, pltpu.roll(total, LANES - d, 1), 0.0)
        return box

    for m in range(8):
        line = m + odd * (7 - 2 * m)
        energy = boxed(m, slice(HEIGHTS, ROWS), 8).sum(axis=0, keepdims=True)
        inverse = 1.0 / (energy + epsilon)
        for k in range(0, HEIGHTS, 64):
            box = boxed(m, slice(k, k + 64), 64) * inverse
            flat_ref[pl.ds(8 * k + line, 64, stride=8), :] = box
    for k in range(0, HEIGHTS, 16):
        out_ref[k : k + 16] = flat_ref[8 * k : 8 * k + 128].reshape(16, 8, LANES).astype(jnp.bfloat16)


def spread():
    column = np.array([-3, -2, -1, 128, 129, 130])
    near = np.abs(column[:, None] - np.arange(LANES)[None, :]) <= 3

    def matrix(position_of, lines, used):
        full = np.zeros((LANES, len(lines), LANES), np.float32)
        for n in used:
            for i, m in enumerate(lines):
                if abs(position_of(n) - m) <= 3:
                    full[6 * n : 6 * n + 6, i] = near
        full = full.reshape(LANES, -1)
        return jnp.asarray(np.concatenate([full, full], axis=0), jnp.bfloat16)

    mid = matrix(lambda n: n, range(8), range(8))
    mo = matrix(lambda n: -1 - n, (0, 1, 2), (0, 1, 2))
    me = matrix(lambda n: 15 - n, (5, 6, 7), (5, 6, 7))
    return mid, mo, me


def steering(wavenumbers):
    waves = jnp.broadcast_to(wavenumbers.reshape(16, 1, 4), (16, 2, 4)).reshape(LANES)
    real = (jnp.arange(LANES) // 4) % 2 == 0
    heights = jnp.arange(HEIGHTS, dtype=jnp.int32).astype(jnp.float32) - jnp.float32(HEIGHTS // 2)
    phases = heights[:, None] * waves[None, :]
    cosine, sine = jnp.cos(phases), jnp.sin(phases)
    full = jnp.concatenate([jnp.where(real, cosine, sine), jnp.where(real, -sine, cosine)], axis=0)
    high = lax.reduce_precision(full, 8, 7)
    low = (full - high).astype(jnp.bfloat16)
    high = high.astype(jnp.bfloat16)
    return jnp.concatenate([high, high, low], axis=1)


VMEM = pl.BlockSpec(memory_space=pltpu.VMEM)


def run(kernel, shape, vmem, flops, scratch=()):
    def call(*operands):
        return pl.pallas_call(
            kernel,
            out_shape=jax.ShapeDtypeStruct(shape, jnp.float32),
            in_specs=[VMEM] * len(operands),
            out_specs=VMEM,
            scratch_shapes=list(scratch),
            compiler_params=pltpu.CompilerParams(vmem_limit_bytes=vmem),
            cost_estimate=pl.CostEstimate(flops=flops, bytes_accessed=1000000, transcendentals=0),
        )(*operands)

    return call


def spectrum(slc_stack, wavenumbers):
    lines = lax.axis_size("line")
    outer = [pair for i in range(1, lines - 1, 2) for pair in ((i, i + 1), (i + 1, i))]
    inner = [pair for i in range(0, lines, 2) for pair in ((i, i + 1), (i + 1, i))]
    steer = steering(wavenumbers)
    stack = slc_stack.reshape(8, 8, -1, LANES).transpose(0, 2, 1, 3).reshape(-1, LANES)
    edge = run(pack_edge, (16, FIRST, 8, LANES), PACK_VMEM, 1000000)(stack)
    rest = run(pack_rest, (16, 9 - FIRST, 8, LANES), PACK_VMEM, 1000000)(stack, steer)
    edge = lax.all_to_all(edge, "acq", 0, 0, tiled=True)
    rest = lax.all_to_all(rest, "acq", 0, 0, tiled=True)
    mid, mo, me = spread()
    side_o = lax.ppermute(edge, "line", outer)
    side_e = lax.ppermute(jnp.concatenate([edge[:, HALO:], rest[:, :3]], axis=1), "line", inner)
    beams = [pltpu.VMEM((2 * HEIGHTS, 2 * LANES), jnp.float32)]
    edge = run(own_kernel, (FIRST, ROWS, LANES), OWN_VMEM, 1000000000, beams)(edge, steer)
    rest = run(own_kernel, (9 - FIRST, ROWS, LANES), OWN_VMEM, 1000000000, beams)(rest, steer)
    return pl.pallas_call(
        box_kernel,
        out_shape=jax.ShapeDtypeStruct((HEIGHTS, 8, LANES), jnp.bfloat16),
        in_specs=[VMEM] * 8,
        out_specs=VMEM,
        scratch_shapes=[
            pltpu.VMEM((2 * HEIGHTS, 2 * LANES), jnp.float32),
            pltpu.VMEM((8, ROWS, LANES), jnp.float32),
            pltpu.VMEM((ROWS, 8 * LANES), jnp.float32),
            pltpu.VMEM((8 * HEIGHTS, LANES), jnp.float32),
        ],
        name="box",
        compiler_params=pltpu.CompilerParams(vmem_limit_bytes=BOX_VMEM),
        cost_estimate=pl.CostEstimate(flops=1000000000, bytes_accessed=2000000, transcendentals=0),
    )(edge, rest, side_o, side_e, steer, mid, mo, me)


def solution(mesh):
    placed = (P(None, "acq", "line", None), P())
    return jax.shard_map(spectrum, mesh=mesh, in_specs=placed, out_specs=P(None, "line", "acq"), check_vma=False)
```

```python
import jax
import jax.numpy as jnp
import numpy as np
from jax import lax
from jax.experimental import pallas as pl
from jax.experimental.pallas import tpu as pltpu
from jax.sharding import PartitionSpec as P


HEIGHTS = 256
ROWS = HEIGHTS + 8
LANES = 128
epsilon = 1e-06

SLOT = {0: 0, 1: 1, 2: 2, 7: 4, 6: 5, 5: 6, 3: 7, 4: 8}
HALO = 3
OWN_LANES = 48
EDGE_LANES = 18
MERGED = 4
EDGE_TILES = 48 + 16 // MERGED


def parity():
    return lax.rem(lax.axis_index("line"), 2)


def pack_kernel(x_ref, out_ref):
    blocks = x_ref.shape[0] // 64
    odd = parity()
    place = OWN_LANES + EDGE_LANES * lax.rem(lax.axis_index("acq"), MERGED)
    lane = lax.broadcasted_iota(jnp.int32, (8, LANES), 1)
    halo = [jnp.zeros((8, LANES), jnp.float32) for _ in range(blocks)]
    for m in range(8):
        line = m + odd * (7 - 2 * m)
        for start in (6 * m, place + 6 * m)[: 2 if m < 3 else 1]:
            left = (lane >= start) & (lane < start + 3)
            right = (lane >= start + 3) & (lane < start + 6)
            for j in range(blocks):
                tile = x_ref[pl.ds(8 * j + line, 8, stride=8 * blocks), :]
                if isinstance(start, int):
                    out_ref[blocks - 1 - j, SLOT[m]] = tile
                moved = pltpu.roll(tile, start + 3, 1)
                if j + 1 < blocks:
                    halo[j + 1] = jnp.where(left, moved, halo[j + 1])
                if j >= 1:
                    halo[j - 1] = jnp.where(right, moved, halo[j - 1])
    for j in range(blocks):
        out_ref[blocks - 1 - j, HALO] = halo[j]


def edge_kernel(r_ref, o_ref, e_ref):
    lane = lax.broadcasted_iota(jnp.int32, (8, LANES), 1)
    for j in range(16):
        for s in range(3):
            o_ref[3 * j + s] = r_ref[j, s]
        for s in range(4):
            e_ref[j, s] = r_ref[j, HALO + s]
    for g in range(16 // MERGED):
        total = r_ref[MERGED * g, HALO]
        for j in range(1, MERGED):
            total = total + r_ref[MERGED * g + j, HALO]
        o_ref[48 + g] = jnp.where(lane < OWN_LANES, 0.0, total)


def beam_pair(first, second, steer_ref, beams_ref):
    both = jnp.concatenate([first.reshape(LANES, LANES), second.reshape(LANES, LANES)], axis=1)
    high = both.astype(jnp.bfloat16)
    low = (both - high.astype(jnp.float32)).astype(jnp.bfloat16)
    stacked = jnp.concatenate([high, low, high], axis=0)
    beams_ref[...] = jnp.dot(steer_ref[...], stacked, preferred_element_type=jnp.float32)
    re, im = beams_ref[:HEIGHTS], beams_ref[HEIGHTS:]
    power = re * re + im * im
    squares = (both * both).reshape(16, 8, 2 * LANES).sum(axis=0)
    return jnp.concatenate([power, squares], axis=0)


def own_kernel(r_ref, steer_ref, out_ref, beams_ref):
    for s in (0, 2, 4, 6, 8):
        t = min(s + 1, 8)
        both = beam_pair(r_ref[:, s], r_ref[:, t], steer_ref, beams_ref)
        out_ref[s] = both[:, :LANES]
        if t != s:
            out_ref[t] = both[:, LANES:]


def halves(field):
    high = field.astype(jnp.bfloat16)
    low = (field - high.astype(jnp.float32)).astype(jnp.bfloat16)
    return jnp.concatenate([high, low], axis=1)


def boxed(total, correction):
    lane = lax.broadcasted_iota(jnp.int32, total.shape, 1)
    box = total + correction
    for d in (1, 2, 3):
        box = box + jnp.where(lane >= d, pltpu.roll(total, d, 1), 0.0)
        box = box + jnp.where(lane < LANES - d, pltpu.roll(total, LANES - d, 1), 0.0)
    return box


def normalize(m, odd, box_of, flat_ref):
    line = m + odd * (7 - 2 * m)
    energy = box_of(m, slice(HEIGHTS, ROWS)).sum(axis=0, keepdims=True)
    inverse = 1.0 / (energy + epsilon)
    for k in range(0, HEIGHTS, 64):
        flat_ref[pl.ds(8 * k + line, 64, stride=8), :] = box_of(m, slice(k, k + 64)) * inverse


def inner_kernel(own_ref, e_ref, steer_ref, mid_ref, me_ref, flat_ref, part_ref, cor_ref, beams_ref, side_ref, all_ref):
    for s in (0, 2):
        both = beam_pair(e_ref[:, s], e_ref[:, s + 1], steer_ref, beams_ref)
        side_ref[s] = both[:, :LANES]
        side_ref[s + 1] = both[:, LANES:]
    all_ref[...] = jnp.dot(halves(own_ref[HALO]), mid_ref[...], preferred_element_type=jnp.float32)
    all_ref[:, 5 * LANES :] += jnp.dot(halves(side_ref[0]), me_ref[...], preferred_element_type=jnp.float32)
    cor_ref[...] = all_ref[:, : 3 * LANES]

    def summed(m, rows):
        total = None
        for position in range(max(m - 3, 0), m + 4):
            term = side_ref[position - 7, rows] if position > 7 else own_ref[SLOT[position], rows]
            total = term if total is None else total + term
        return total

    for m in range(3):
        for k in range(0, ROWS, 88):
            part_ref[m, k : k + 88] = summed(m, slice(k, k + 88))
    odd = parity()
    for m in range(3, 8):
        normalize(m, odd, lambda m, rows: boxed(summed(m, rows), all_ref[rows, m * LANES : (m + 1) * LANES]), flat_ref)


def outer_kernel(o_ref, part_ref, cor_ref, flat_ref, steer_ref, mo_ref, out_ref, beams_ref, side_ref, halo_ref, all_ref, edge_ref, done_ref, sems):
    lane = lax.broadcasted_iota(jnp.int32, (8, LANES), 1)
    for j in range(16):
        start = OWN_LANES + EDGE_LANES * ((15 - j) % MERGED)
        halo_ref[j] = jnp.where(lane < EDGE_LANES, pltpu.roll(o_ref[48 + j // MERGED], LANES - start, 1), 0.0)
    lines = o_ref[:48].reshape(16, 3, 8, LANES)
    for s in (0, 2):
        both = beam_pair(lines[:, s], lines[:, 1] if s == 0 else halo_ref[...], steer_ref, beams_ref)
        side_ref[s] = both[:, :LANES]
        side_ref[s + 1] = both[:, LANES:]
    all_ref[...] = cor_ref[...] + jnp.dot(halves(side_ref[3]), mo_ref[...], preferred_element_type=jnp.float32)

    def box_of(m, rows):
        total = part_ref[m, rows]
        for i in range(3 - m):
            total = total + side_ref[i, rows]
        return boxed(total, all_ref[rows, m * LANES : (m + 1) * LANES])

    odd = parity()
    for m in range(3):
        normalize(m, odd, box_of, edge_ref)
    sub = lax.broadcasted_iota(jnp.int32, (16, 8, LANES), 1)
    edge = jnp.where(odd == 1, 7 - sub, sub) < 3
    copies = []
    for q in range(4):
        for k in range(64 * q, 64 * q + 64, 16):
            rows = slice(8 * k, 8 * k + 128)
            merged = jnp.where(edge, edge_ref[rows].reshape(16, 8, LANES), flat_ref[rows].reshape(16, 8, LANES))
            done_ref[k : k + 16] = merged.astype(jnp.bfloat16)
        copy = pltpu.make_async_copy(done_ref.at[pl.ds(64 * q, 64)], out_ref.at[pl.ds(64 * q, 64)], sems.at[q])
        copy.start()
        copies.append(copy)
    for copy in copies:
        copy.wait()


def spread():
    column = np.array([-3, -2, -1, 128, 129, 130])
    near = np.abs(column[:, None] - np.arange(LANES)[None, :]) <= 3

    def matrix(position_of, lines, used):
        full = np.zeros((LANES, len(lines), LANES), np.float32)
        for n in used:
            for i, m in enumerate(lines):
                if abs(position_of(n) - m) <= 3:
                    full[6 * n : 6 * n + 6, i] = near
        full = full.reshape(LANES, -1)
        return jnp.asarray(np.concatenate([full, full], axis=0), jnp.bfloat16)

    mid = matrix(lambda n: n, range(8), range(8))
    mo = matrix(lambda n: -1 - n, (0, 1, 2), (0, 1, 2))
    me = matrix(lambda n: 15 - n, (5, 6, 7), (5, 6, 7))
    return mid, mo, me


def steering(wavenumbers):
    waves = jnp.broadcast_to(wavenumbers.reshape(16, 1, 4)[::-1], (16, 2, 4)).reshape(LANES)
    real = (jnp.arange(LANES) // 4) % 2 == 0
    heights = jnp.arange(HEIGHTS, dtype=jnp.int32).astype(jnp.float32) - jnp.float32(HEIGHTS // 2)
    phases = heights[:, None] * waves[None, :]
    cosine, sine = jnp.cos(phases), jnp.sin(phases)
    full = jnp.concatenate([jnp.where(real, cosine, sine), jnp.where(real, -sine, cosine)], axis=0)
    high = lax.reduce_precision(full, 8, 7)
    low = (full - high).astype(jnp.bfloat16)
    high = high.astype(jnp.bfloat16)
    return jnp.concatenate([high, high, low], axis=1)


VMEM = pl.BlockSpec(memory_space=pltpu.VMEM)
ANY = pl.BlockSpec(memory_space=pl.ANY)


def call(kernel, shapes, vmem, flops, scratch=(), out=VMEM, dtype=jnp.float32):
    def on(*operands):
        return pl.pallas_call(
            kernel,
            out_shape=[jax.ShapeDtypeStruct(shape, dtype) for shape in shapes],
            in_specs=[VMEM] * len(operands),
            out_specs=[out] * len(shapes),
            scratch_shapes=list(scratch),
            compiler_params=pltpu.CompilerParams(vmem_limit_bytes=vmem << 20),
            cost_estimate=pl.CostEstimate(flops=flops, bytes_accessed=1000000, transcendentals=0),
        )(*operands)

    return on


def spectrum(slc_stack, wavenumbers):
    lines, acqs = lax.axis_size("line"), lax.axis_size("acq")
    outer = [pair for i in range(1, lines - 1, 2) for pair in ((i, i + 1), (i + 1, i))]
    inner = [pair for i in range(0, lines, 2) for pair in ((i, i + 1), (i + 1, i))]
    beams = pltpu.VMEM((2 * HEIGHTS, 2 * LANES), jnp.float32)
    stack = slc_stack.reshape(8, 8, -1, LANES).transpose(0, 2, 1, 3).reshape(-1, LANES)
    (packed,) = call(pack_kernel, [(16, 9, 8, LANES)], 4, 1000000)(stack)
    gathered = lax.all_to_all(packed, "acq", 0, 0, tiled=True, axis_index_groups=[list(range(acqs))[::-1]])
    steer = steering(wavenumbers)
    mid, mo, me = spread()
    to_o, to_e = call(edge_kernel, [(EDGE_TILES, 8, LANES), (16, 4, 8, LANES)], 4, 1000000)(gathered)
    side_o = lax.ppermute(to_o, "line", outer)
    side_e = lax.ppermute(to_e, "line", inner)
    (own,) = call(own_kernel, [(9, ROWS, LANES)], 10, 1000000000, [beams])(gathered, steer)
    flat, part, cor = call(
        inner_kernel,
        [(8 * HEIGHTS, LANES), (3, ROWS, LANES), (ROWS, 3 * LANES)],
        14,
        1000000000,
        [beams, pltpu.VMEM((4, ROWS, LANES), jnp.float32), pltpu.VMEM((ROWS, 8 * LANES), jnp.float32)],
    )(own, side_e, steer, mid, me)
    (result,) = call(
        outer_kernel,
        [(HEIGHTS, 8, LANES)],
        12,
        1000000000,
        [
            beams,
            pltpu.VMEM((4, ROWS, LANES), jnp.float32),
            pltpu.VMEM((16, 8, LANES), jnp.float32),
            pltpu.VMEM((ROWS, 3 * LANES), jnp.float32),
            pltpu.VMEM((8 * HEIGHTS, LANES), jnp.float32),
            pltpu.VMEM((HEIGHTS, 8, LANES), jnp.bfloat16),
            pltpu.SemaphoreType.DMA((4,)),
        ],
        out=ANY,
        dtype=jnp.bfloat16,
    )(side_o, part, cor, flat, steer, mo)
    return result


def solution(mesh):
    placed = (P(None, "acq", "line", None), P())
    return jax.shard_map(spectrum, mesh=mesh, in_specs=placed, out_specs=P(None, "line", "acq"), check_vma=False)
```

```python
import jax
import jax.numpy as jnp
import numpy as np
from jax import lax
from jax.experimental import pallas as pl
from jax.experimental.pallas import tpu as pltpu
from jax.sharding import PartitionSpec as P


HEIGHTS = 256
ROWS = HEIGHTS + 8
LANES = 128
epsilon = 1e-06

SLOT = {0: 0, 1: 1, 2: 2, 7: 4, 6: 5, 5: 6, 3: 7, 4: 8}
HALO = 3
OWN_LANES = 48
EDGE_LANES = 18
MERGED = 4
EDGE_TILES = 48 + 16 // MERGED
PIECES = 4
PLACE = [2 * z + y for z in (4, 3, 5, 2, 6, 1, 7, 0) for y in (0, 1)]
MERGE = [acq % MERGED for acq in PLACE]


def parity():
    return lax.rem(lax.axis_index("line"), 2)


def pack_kernel(x_hbm, out_hbm, x_ref, out_ref, in_sems, out_sems):
    blocks = x_ref.shape[0] // 64
    step = blocks // PIECES
    wide = x_ref.reshape(8, 8 * blocks, LANES)
    loads = []
    for q in range(PIECES):
        rows = pl.ds(8 * step * q, 8 * step)
        loads.append(pltpu.make_async_copy(x_hbm.at[:, rows], wide.at[:, rows], in_sems.at[q]))
        loads[q].start()
    odd = parity()
    place = OWN_LANES + EDGE_LANES * lax.rem(lax.axis_index("acq"), MERGED)
    lane = lax.broadcasted_iota(jnp.int32, (8, LANES), 1)
    zero = jnp.zeros((8, LANES), jnp.float32)
    halo = [zero, zero]
    stores = []
    for q in range(PIECES):
        loads[q].wait()
        for j in range(step * q, step * q + step):
            halo.append(zero)
            for m in range(8):
                line = m + odd * (7 - 2 * m)
                tile = x_ref[pl.ds(8 * j + line, 8, stride=8 * blocks), :]
                out_ref[PLACE.index(j), SLOT[m]] = tile
                for start in (6 * m, place + 6 * m)[: 2 if m < 3 else 1]:
                    left = (lane >= start) & (lane < start + 3)
                    right = (lane >= start + 3) & (lane < start + 6)
                    moved = pltpu.roll(tile, start + 3, 1)
                    halo[j + 2] = jnp.where(left, moved, halo[j + 2])
                    halo[j] = jnp.where(right, moved, halo[j])
        ready = range(max(step * q - 1, 0), step * q + step - 1 if q < PIECES - 1 else blocks)
        for j in ready:
            n = PLACE.index(j)
            out_ref[n, HALO] = halo[j + 1]
            stores.append(pltpu.make_async_copy(out_ref.at[n], out_hbm.at[n], out_sems.at[j]))
            stores[-1].start()
    for store in stores:
        store.wait()


def edge_kernel(r_ref, o_ref, e_ref):
    lane = lax.broadcasted_iota(jnp.int32, (8, LANES), 1)
    for j in range(16):
        for s in range(3):
            o_ref[3 * j + s] = r_ref[j, s]
        for s in range(4):
            e_ref[j, s] = r_ref[j, HALO + s]
    for g in range(16 // MERGED):
        total = r_ref[MERGED * g, HALO]
        for j in range(1, MERGED):
            total = total + r_ref[MERGED * g + j, HALO]
        o_ref[48 + g] = jnp.where(lane < OWN_LANES, 0.0, total)


def beam_pair(first, second, steer_ref, beams_ref):
    both = jnp.concatenate([first.reshape(LANES, LANES), second.reshape(LANES, LANES)], axis=1)
    high = both.astype(jnp.bfloat16)
    low = (both - high.astype(jnp.float32)).astype(jnp.bfloat16)
    stacked = jnp.concatenate([high, low, high], axis=0)
    beams_ref[...] = jnp.dot(steer_ref[...], stacked, preferred_element_type=jnp.float32)
    re, im = beams_ref[:HEIGHTS], beams_ref[HEIGHTS:]
    power = re * re + im * im
    squares = (both * both).reshape(16, 8, 2 * LANES).sum(axis=0)
    return jnp.concatenate([power, squares], axis=0)


def own_kernel(r_ref, steer_ref, out_ref, beams_ref):
    for s in (0, 2, 4, 6, 8):
        t = min(s + 1, 8)
        both = beam_pair(r_ref[:, s], r_ref[:, t], steer_ref, beams_ref)
        out_ref[s] = both[:, :LANES]
        if t != s:
            out_ref[t] = both[:, LANES:]


def halves(field):
    high = field.astype(jnp.bfloat16)
    low = (field - high.astype(jnp.float32)).astype(jnp.bfloat16)
    return jnp.concatenate([high, low], axis=1)


def boxed(total, correction):
    lane = lax.broadcasted_iota(jnp.int32, total.shape, 1)
    box = total + correction
    for d in (1, 2, 3):
        box = box + jnp.where(lane >= d, pltpu.roll(total, d, 1), 0.0)
        box = box + jnp.where(lane < LANES - d, pltpu.roll(total, LANES - d, 1), 0.0)
    return box


def normalize(m, odd, box_of, flat_ref):
    line = m + odd * (7 - 2 * m)
    energy = box_of(m, slice(HEIGHTS, ROWS)).sum(axis=0, keepdims=True)
    inverse = 1.0 / (energy + epsilon)
    for k in range(0, HEIGHTS, 64):
        flat_ref[pl.ds(8 * k + line, 64, stride=8), :] = box_of(m, slice(k, k + 64)) * inverse


def inner_kernel(own_ref, e_ref, steer_ref, mid_ref, me_ref, flat_ref, part_ref, cor_ref, beams_ref, side_ref, all_ref):
    for s in (0, 2):
        both = beam_pair(e_ref[:, s], e_ref[:, s + 1], steer_ref, beams_ref)
        side_ref[s] = both[:, :LANES]
        side_ref[s + 1] = both[:, LANES:]
    all_ref[...] = jnp.dot(halves(own_ref[HALO]), mid_ref[...], preferred_element_type=jnp.float32)
    all_ref[:, 5 * LANES :] += jnp.dot(halves(side_ref[0]), me_ref[...], preferred_element_type=jnp.float32)
    cor_ref[...] = all_ref[:, : 3 * LANES]

    def summed(m, rows):
        total = None
        for position in range(max(m - 3, 0), m + 4):
            term = side_ref[position - 7, rows] if position > 7 else own_ref[SLOT[position], rows]
            total = term if total is None else total + term
        return total

    for m in range(3):
        for k in range(0, ROWS, 88):
            part_ref[m, k : k + 88] = summed(m, slice(k, k + 88))
    odd = parity()
    for m in range(3, 8):
        normalize(m, odd, lambda m, rows: boxed(summed(m, rows), all_ref[rows, m * LANES : (m + 1) * LANES]), flat_ref)


def outer_kernel(o_ref, part_ref, cor_ref, flat_ref, steer_ref, mo_ref, out_ref, beams_ref, side_ref, halo_ref, all_ref, edge_ref, done_ref, sems):
    lane = lax.broadcasted_iota(jnp.int32, (8, LANES), 1)
    for j in range(16):
        start = OWN_LANES + EDGE_LANES * MERGE[j]
        halo_ref[j] = jnp.where(lane < EDGE_LANES, pltpu.roll(o_ref[48 + j // MERGED], LANES - start, 1), 0.0)
    lines = o_ref[:48].reshape(16, 3, 8, LANES)
    for s in (0, 2):
        both = beam_pair(lines[:, s], lines[:, 1] if s == 0 else halo_ref[...], steer_ref, beams_ref)
        side_ref[s] = both[:, :LANES]
        side_ref[s + 1] = both[:, LANES:]
    all_ref[...] = cor_ref[...] + jnp.dot(halves(side_ref[3]), mo_ref[...], preferred_element_type=jnp.float32)

    def box_of(m, rows):
        total = part_ref[m, rows]
        for i in range(3 - m):
            total = total + side_ref[i, rows]
        return boxed(total, all_ref[rows, m * LANES : (m + 1) * LANES])

    odd = parity()
    for m in range(3):
        normalize(m, odd, box_of, edge_ref)
    sub = lax.broadcasted_iota(jnp.int32, (16, 8, LANES), 1)
    edge = jnp.where(odd == 1, 7 - sub, sub) < 3
    copies = []
    for q in range(4):
        for k in range(64 * q, 64 * q + 64, 16):
            rows = slice(8 * k, 8 * k + 128)
            merged = jnp.where(edge, edge_ref[rows].reshape(16, 8, LANES), flat_ref[rows].reshape(16, 8, LANES))
            done_ref[k : k + 16] = merged.astype(jnp.bfloat16)
        copy = pltpu.make_async_copy(done_ref.at[pl.ds(64 * q, 64)], out_ref.at[pl.ds(64 * q, 64)], sems.at[q])
        copy.start()
        copies.append(copy)
    for copy in copies:
        copy.wait()


def spread():
    column = np.array([-3, -2, -1, 128, 129, 130])
    near = np.abs(column[:, None] - np.arange(LANES)[None, :]) <= 3

    def matrix(position_of, lines, used):
        full = np.zeros((LANES, len(lines), LANES), np.float32)
        for n in used:
            for i, m in enumerate(lines):
                if abs(position_of(n) - m) <= 3:
                    full[6 * n : 6 * n + 6, i] = near
        full = full.reshape(LANES, -1)
        return jnp.asarray(np.concatenate([full, full], axis=0), jnp.bfloat16)

    mid = matrix(lambda n: n, range(8), range(8))
    mo = matrix(lambda n: -1 - n, (0, 1, 2), (0, 1, 2))
    me = matrix(lambda n: 15 - n, (5, 6, 7), (5, 6, 7))
    return mid, mo, me


def steering(wavenumbers):
    planes = wavenumbers.reshape(8, 8)
    ordered = jnp.stack([planes[4:], planes[:4][::-1]], axis=1).reshape(16, 1, 4)
    waves = jnp.broadcast_to(ordered, (16, 2, 4)).reshape(LANES)
    real = (jnp.arange(LANES) // 4) % 2 == 0
    heights = jnp.arange(HEIGHTS, dtype=jnp.int32).astype(jnp.float32) - jnp.float32(HEIGHTS // 2)
    phases = heights[:, None] * waves[None, :]
    cosine, sine = jnp.cos(phases), jnp.sin(phases)
    full = jnp.concatenate([jnp.where(real, cosine, sine), jnp.where(real, -sine, cosine)], axis=0)
    high = lax.reduce_precision(full, 8, 7)
    low = (full - high).astype(jnp.bfloat16)
    high = high.astype(jnp.bfloat16)
    return jnp.concatenate([high, high, low], axis=1)


VMEM = pl.BlockSpec(memory_space=pltpu.VMEM)
ANY = pl.BlockSpec(memory_space=pl.ANY)


def call(kernel, shapes, vmem, flops, scratch=(), out=VMEM, dtype=jnp.float32, into=VMEM):
    def on(*operands):
        return pl.pallas_call(
            kernel,
            out_shape=[jax.ShapeDtypeStruct(shape, dtype) for shape in shapes],
            in_specs=[into] * len(operands),
            out_specs=[out] * len(shapes),
            scratch_shapes=list(scratch),
            compiler_params=pltpu.CompilerParams(vmem_limit_bytes=vmem << 20),
            cost_estimate=pl.CostEstimate(flops=flops, bytes_accessed=1000000, transcendentals=0),
        )(*operands)

    return on


def spectrum(slc_stack, wavenumbers):
    lines = lax.axis_size("line")
    outer = [pair for i in range(1, lines - 1, 2) for pair in ((i, i + 1), (i + 1, i))]
    inner = [pair for i in range(0, lines, 2) for pair in ((i, i + 1), (i + 1, i))]
    beams = pltpu.VMEM((2 * HEIGHTS, 2 * LANES), jnp.float32)
    stack = slc_stack.reshape(8, 8, -1, LANES).transpose(0, 2, 1, 3).reshape(8, -1, LANES)
    (packed,) = call(
        pack_kernel,
        [(16, 9, 8, LANES)],
        60,
        1000000,
        [
            pltpu.VMEM((1024, LANES), jnp.float32),
            pltpu.VMEM((16, 9, 8, LANES), jnp.float32),
            pltpu.SemaphoreType.DMA((PIECES,)),
            pltpu.SemaphoreType.DMA((16,)),
        ],
        out=ANY,
        into=ANY,
    )(stack)
    gathered = lax.all_to_all(packed, "acq", 0, 0, tiled=True, axis_index_groups=[PLACE])
    steer = steering(wavenumbers)
    mid, mo, me = spread()
    to_o, to_e = call(edge_kernel, [(EDGE_TILES, 8, LANES), (16, 4, 8, LANES)], 4, 1000000)(gathered)
    side_o = lax.ppermute(to_o, "line", outer)
    side_e = lax.ppermute(to_e, "line", inner)
    (own,) = call(own_kernel, [(9, ROWS, LANES)], 10, 1000000000, [beams])(gathered, steer)
    flat, part, cor = call(
        inner_kernel,
        [(8 * HEIGHTS, LANES), (3, ROWS, LANES), (ROWS, 3 * LANES)],
        14,
        1000000000,
        [beams, pltpu.VMEM((4, ROWS, LANES), jnp.float32), pltpu.VMEM((ROWS, 8 * LANES), jnp.float32)],
    )(own, side_e, steer, mid, me)
    (result,) = call(
        outer_kernel,
        [(HEIGHTS, 8, LANES)],
        12,
        1000000000,
        [
            beams,
            pltpu.VMEM((4, ROWS, LANES), jnp.float32),
            pltpu.VMEM((16, 8, LANES), jnp.float32),
            pltpu.VMEM((ROWS, 3 * LANES), jnp.float32),
            pltpu.VMEM((8 * HEIGHTS, LANES), jnp.float32),
            pltpu.VMEM((HEIGHTS, 8, LANES), jnp.bfloat16),
            pltpu.SemaphoreType.DMA((4,)),
        ],
        out=ANY,
        dtype=jnp.bfloat16,
    )(side_o, part, cor, flat, steer, mo)
    return result


def solution(mesh):
    placed = (P(None, "acq", "line", None), P())
    return jax.shard_map(spectrum, mesh=mesh, in_specs=placed, out_specs=P(None, "line", "acq"), check_vma=False)
```

```python
import jax
import jax.numpy as jnp
import numpy as np
from jax import lax
from jax.experimental import pallas as pl
from jax.experimental.pallas import tpu as pltpu
from jax.sharding import PartitionSpec as P


HEIGHTS = 256
ROWS = HEIGHTS + 8
LANES = 128
epsilon = 1e-06

SLOT = {0: 0, 1: 1, 2: 2, 7: 4, 6: 5, 5: 6, 3: 7, 4: 8}
HALO = 3
OWN_LANES = 48
EDGE_LANES = 18
MERGED = 4
EDGE_TILES = 48 + 16 // MERGED
PLACE = [2 * z + y for z in (4, 3, 5, 2, 6, 1, 7, 0) for y in (0, 1)]
MERGE = [acq % MERGED for acq in PLACE]


def parity():
    return lax.rem(lax.axis_index("line"), 2)


def pack_kernel(x_ref, out_ref):
    blocks = x_ref.shape[0] // 64
    odd = parity()
    place = OWN_LANES + EDGE_LANES * lax.rem(lax.axis_index("acq"), MERGED)
    lane = lax.broadcasted_iota(jnp.int32, (8, LANES), 1)
    zero = jnp.zeros((8, LANES), jnp.float32)
    halo = [zero, zero]
    for j in range(blocks):
        halo.append(zero)
        for m in range(8):
            line = m + odd * (7 - 2 * m)
            tile = x_ref[pl.ds(8 * j + line, 8, stride=8 * blocks), :]
            out_ref[PLACE.index(j), SLOT[m]] = tile
            for start in (6 * m, place + 6 * m)[: 2 if m < 3 else 1]:
                left = (lane >= start) & (lane < start + 3)
                right = (lane >= start + 3) & (lane < start + 6)
                moved = pltpu.roll(tile, start + 3, 1)
                halo[j + 2] = jnp.where(left, moved, halo[j + 2])
                halo[j] = jnp.where(right, moved, halo[j])
    for j in range(blocks):
        out_ref[PLACE.index(j), HALO] = halo[j + 1]


def edge_kernel(r_ref, o_ref, e_ref):
    lane = lax.broadcasted_iota(jnp.int32, (8, LANES), 1)
    for j in range(16):
        for s in range(3):
            o_ref[3 * j + s] = r_ref[j, s]
        for s in range(4):
            e_ref[j, s] = r_ref[j, HALO + s]
    for g in range(16 // MERGED):
        total = r_ref[MERGED * g, HALO]
        for j in range(1, MERGED):
            total = total + r_ref[MERGED * g + j, HALO]
        o_ref[48 + g] = jnp.where(lane < OWN_LANES, 0.0, total)


def beam_pair(first, second, steer_ref, beams_ref):
    both = jnp.concatenate([first.reshape(LANES, LANES), second.reshape(LANES, LANES)], axis=1)
    high = both.astype(jnp.bfloat16)
    low = (both - high.astype(jnp.float32)).astype(jnp.bfloat16)
    stacked = jnp.concatenate([high, low, high], axis=0)
    beams_ref[...] = jnp.dot(steer_ref[...], stacked, preferred_element_type=jnp.float32)
    re, im = beams_ref[:HEIGHTS], beams_ref[HEIGHTS:]
    power = re * re + im * im
    squares = (both * both).reshape(16, 8, 2 * LANES).sum(axis=0)
    return jnp.concatenate([power, squares], axis=0)


def own_kernel(r_ref, steer_ref, out_ref, beams_ref):
    for s in (0, 2, 4, 6, 8):
        t = min(s + 1, 8)
        both = beam_pair(r_ref[:, s], r_ref[:, t], steer_ref, beams_ref)
        out_ref[s] = both[:, :LANES]
        if t != s:
            out_ref[t] = both[:, LANES:]


def halves(field):
    high = field.astype(jnp.bfloat16)
    low = (field - high.astype(jnp.float32)).astype(jnp.bfloat16)
    return jnp.concatenate([high, low], axis=1)


def boxed(total, correction):
    lane = lax.broadcasted_iota(jnp.int32, total.shape, 1)
    box = total + correction
    for d in (1, 2, 3):
        box = box + jnp.where(lane >= d, pltpu.roll(total, d, 1), 0.0)
        box = box + jnp.where(lane < LANES - d, pltpu.roll(total, LANES - d, 1), 0.0)
    return box


def normalize(m, odd, box_of, flat_ref):
    line = m + odd * (7 - 2 * m)
    energy = box_of(m, slice(HEIGHTS, ROWS)).sum(axis=0, keepdims=True)
    inverse = 1.0 / (energy + epsilon)
    for k in range(0, HEIGHTS, 64):
        flat_ref[pl.ds(8 * k + line, 64, stride=8), :] = box_of(m, slice(k, k + 64)) * inverse


def inner_kernel(own_ref, e_ref, steer_ref, mid_ref, me_ref, flat_ref, part_ref, cor_ref, beams_ref, side_ref, all_ref):
    for s in (0, 2):
        both = beam_pair(e_ref[:, s], e_ref[:, s + 1], steer_ref, beams_ref)
        side_ref[s] = both[:, :LANES]
        side_ref[s + 1] = both[:, LANES:]
    all_ref[...] = jnp.dot(halves(own_ref[HALO]), mid_ref[...], preferred_element_type=jnp.float32)
    all_ref[:, 5 * LANES :] += jnp.dot(halves(side_ref[0]), me_ref[...], preferred_element_type=jnp.float32)
    cor_ref[...] = all_ref[:, : 3 * LANES]

    def summed(m, rows):
        total = None
        for position in range(max(m - 3, 0), m + 4):
            term = side_ref[position - 7, rows] if position > 7 else own_ref[SLOT[position], rows]
            total = term if total is None else total + term
        return total

    for m in range(3):
        for k in range(0, ROWS, 88):
            part_ref[m, k : k + 88] = summed(m, slice(k, k + 88))
    odd = parity()
    for m in range(3, 8):
        normalize(m, odd, lambda m, rows: boxed(summed(m, rows), all_ref[rows, m * LANES : (m + 1) * LANES]), flat_ref)


def outer_kernel(o_ref, part_ref, cor_ref, flat_ref, steer_ref, mo_ref, out_ref, beams_ref, side_ref, halo_ref, all_ref, edge_ref, done_ref, sems):
    lane = lax.broadcasted_iota(jnp.int32, (8, LANES), 1)
    for j in range(16):
        start = OWN_LANES + EDGE_LANES * MERGE[j]
        halo_ref[j] = jnp.where(lane < EDGE_LANES, pltpu.roll(o_ref[48 + j // MERGED], LANES - start, 1), 0.0)
    lines = o_ref[:48].reshape(16, 3, 8, LANES)
    for s in (0, 2):
        both = beam_pair(lines[:, s], lines[:, 1] if s == 0 else halo_ref[...], steer_ref, beams_ref)
        side_ref[s] = both[:, :LANES]
        side_ref[s + 1] = both[:, LANES:]
    all_ref[...] = cor_ref[...] + jnp.dot(halves(side_ref[3]), mo_ref[...], preferred_element_type=jnp.float32)

    def box_of(m, rows):
        total = part_ref[m, rows]
        for i in range(3 - m):
            total = total + side_ref[i, rows]
        return boxed(total, all_ref[rows, m * LANES : (m + 1) * LANES])

    odd = parity()
    for m in range(3):
        normalize(m, odd, box_of, edge_ref)
    sub = lax.broadcasted_iota(jnp.int32, (16, 8, LANES), 1)
    edge = jnp.where(odd == 1, 7 - sub, sub) < 3
    copies = []
    for q in range(4):
        for k in range(64 * q, 64 * q + 64, 16):
            rows = slice(8 * k, 8 * k + 128)
            merged = jnp.where(edge, edge_ref[rows].reshape(16, 8, LANES), flat_ref[rows].reshape(16, 8, LANES))
            done_ref[k : k + 16] = merged.astype(jnp.bfloat16)
        copy = pltpu.make_async_copy(done_ref.at[pl.ds(64 * q, 64)], out_ref.at[pl.ds(64 * q, 64)], sems.at[q])
        copy.start()
        copies.append(copy)
    for copy in copies:
        copy.wait()


def spread():
    column = np.array([-3, -2, -1, 128, 129, 130])
    near = np.abs(column[:, None] - np.arange(LANES)[None, :]) <= 3

    def matrix(position_of, lines, used):
        full = np.zeros((LANES, len(lines), LANES), np.float32)
        for n in used:
            for i, m in enumerate(lines):
                if abs(position_of(n) - m) <= 3:
                    full[6 * n : 6 * n + 6, i] = near
        full = full.reshape(LANES, -1)
        return jnp.asarray(np.concatenate([full, full], axis=0), jnp.bfloat16)

    mid = matrix(lambda n: n, range(8), range(8))
    mo = matrix(lambda n: -1 - n, (0, 1, 2), (0, 1, 2))
    me = matrix(lambda n: 15 - n, (5, 6, 7), (5, 6, 7))
    return mid, mo, me


def steering(wavenumbers):
    source = np.array([4 * acq + k for acq in PLACE for _ in range(2) for k in range(4)])
    chosen = np.arange(len(source) // 2)[:, None] == source[None, :]
    waves = jnp.sum(jnp.where(chosen, wavenumbers[:, None], 0.0), axis=0)
    real = (np.arange(LANES) // 4) % 2 == 0
    heights = np.arange(HEIGHTS, dtype=np.float32) - np.float32(HEIGHTS // 2)
    phases = jnp.asarray(heights)[:, None] * waves[None, :]
    cosine, sine = jnp.cos(phases), jnp.sin(phases)
    full = jnp.concatenate([jnp.where(real, cosine, sine), jnp.where(real, -sine, cosine)], axis=0)
    high = lax.reduce_precision(full, 8, 7)
    low = (full - high).astype(jnp.bfloat16)
    high = high.astype(jnp.bfloat16)
    return jnp.concatenate([high, high, low], axis=1)


VMEM = pl.BlockSpec(memory_space=pltpu.VMEM)
ANY = pl.BlockSpec(memory_space=pl.ANY)


def call(kernel, shapes, vmem, flops, scratch=(), out=VMEM, dtype=jnp.float32):
    def on(*operands):
        return pl.pallas_call(
            kernel,
            out_shape=[jax.ShapeDtypeStruct(shape, dtype) for shape in shapes],
            in_specs=[VMEM] * len(operands),
            out_specs=[out] * len(shapes),
            scratch_shapes=list(scratch),
            compiler_params=pltpu.CompilerParams(vmem_limit_bytes=vmem << 20),
            cost_estimate=pl.CostEstimate(flops=flops, bytes_accessed=1000000, transcendentals=0),
        )(*operands)

    return on


def spectrum(slc_stack, wavenumbers):
    lines = lax.axis_size("line")
    outer = [pair for i in range(1, lines - 1, 2) for pair in ((i, i + 1), (i + 1, i))]
    inner = [pair for i in range(0, lines, 2) for pair in ((i, i + 1), (i + 1, i))]
    beams = pltpu.VMEM((2 * HEIGHTS, 2 * LANES), jnp.float32)
    stack = slc_stack.reshape(8, 8, -1, LANES).transpose(0, 2, 1, 3).reshape(-1, LANES)
    (packed,) = call(pack_kernel, [(16, 9, 8, LANES)], 2, 1000000)(stack)
    gathered = lax.all_to_all(packed, "acq", 0, 0, tiled=True, axis_index_groups=[PLACE])
    mid, mo, me = spread()
    to_o, to_e = call(edge_kernel, [(EDGE_TILES, 8, LANES), (16, 4, 8, LANES)], 4, 1000000)(gathered)
    to_o, to_e, wavenumbers = lax.optimization_barrier((to_o, to_e, wavenumbers))
    steer = steering(wavenumbers)
    side_o = lax.ppermute(to_o, "line", outer)
    side_e = lax.ppermute(to_e, "line", inner)
    (own,) = call(own_kernel, [(9, ROWS, LANES)], 10, 1000000000, [beams])(gathered, steer)
    flat, part, cor = call(
        inner_kernel,
        [(8 * HEIGHTS, LANES), (3, ROWS, LANES), (ROWS, 3 * LANES)],
        14,
        1000000000,
        [beams, pltpu.VMEM((4, ROWS, LANES), jnp.float32), pltpu.VMEM((ROWS, 8 * LANES), jnp.float32)],
    )(own, side_e, steer, mid, me)
    (result,) = call(
        outer_kernel,
        [(HEIGHTS, 8, LANES)],
        12,
        1000000000,
        [
            beams,
            pltpu.VMEM((4, ROWS, LANES), jnp.float32),
            pltpu.VMEM((16, 8, LANES), jnp.float32),
            pltpu.VMEM((ROWS, 3 * LANES), jnp.float32),
            pltpu.VMEM((8 * HEIGHTS, LANES), jnp.float32),
            pltpu.VMEM((HEIGHTS, 8, LANES), jnp.bfloat16),
            pltpu.SemaphoreType.DMA((4,)),
        ],
        out=ANY,
        dtype=jnp.bfloat16,
    )(side_o, part, cor, flat, steer, mo)
    return result


def solution(mesh):
    placed = (P(None, "acq", "line", None), P())
    return jax.shard_map(spectrum, mesh=mesh, in_specs=placed, out_specs=P(None, "line", "acq"), check_vma=False)
```

```python
import jax
import jax.numpy as jnp
import numpy as np
from jax import lax
from jax.experimental import pallas as pl
from jax.experimental.pallas import tpu as pltpu
from jax.sharding import PartitionSpec as P


HEIGHTS = 256
ROWS = HEIGHTS + 8
LANES = 128
epsilon = 1e-06

ROW = {0: 0, 1: 8, 2: 16, 7: 28, 6: 36, 5: 44, 3: 52, 4: 60}
HALO_ROW = 24
BLOCK = 68
SLOT = {0: 0, 1: 1, 2: 2, 7: 4, 6: 5, 5: 6, 3: 7, 4: 8}
HALO = 3
EDGE_LANES = 18
MERGED = 7
EDGE_TILES = 48 + 3
PLACE = [2 * z + y for z in (4, 3, 5, 2, 6, 1, 7, 0) for y in (0, 1)]


def parity():
    return lax.rem(lax.axis_index("line"), 2)


def pack_kernel(x_ref, out_ref):
    blocks = x_ref.shape[0] // 64
    odd = parity()
    lane = lax.broadcasted_iota(jnp.int32, (8, LANES), 1)
    zero = jnp.zeros((8, LANES), jnp.float32)
    halo = [zero, zero]
    for j in range(blocks):
        halo.append(zero)
        for m in range(8):
            line = m + odd * (7 - 2 * m)
            tile = x_ref[pl.ds(8 * j + line, 8, stride=8 * blocks), :]
            out_ref[pl.ds(BLOCK * PLACE.index(j) + ROW[m], 8), :] = tile
            left = (lane >= 6 * m) & (lane < 6 * m + 3)
            right = (lane >= 6 * m + 3) & (lane < 6 * m + 6)
            moved = pltpu.roll(tile, 6 * m + 3, 1)
            halo[j + 2] = jnp.where(left, moved, halo[j + 2])
            halo[j] = jnp.where(right, moved, halo[j])
    for j in range(blocks):
        tile = halo[j + 1]
        tile = tile + pltpu.roll(pltpu.roll(tile, 4, 0), LANES // 2, 1)
        out_ref[pl.ds(BLOCK * PLACE.index(j) + HALO_ROW, 4), :] = tile[:4]


def edge_kernel(r_ref, o_ref, e_ref, halo_ref):
    lane = lax.broadcasted_iota(jnp.int32, (8, LANES), 1)
    sub = lax.broadcasted_iota(jnp.int32, (8, LANES), 0)
    for g in range(3):
        sums = [jnp.zeros((8, LANES), jnp.float32) for _ in range(2)]
        for i in range(min(MERGED, 16 - MERGED * g)):
            j = MERGED * g + i
            tile = r_ref[pl.ds(BLOCK * j + HALO_ROW, 8), :]
            tile = jnp.where(sub < 4, tile, pltpu.roll(pltpu.roll(tile, 4, 0), LANES // 2, 1))
            tile = jnp.where(lane < 48, tile, 0.0)
            halo_ref[j] = tile
            here = (lane >= EDGE_LANES * i) & (lane < EDGE_LANES * (i + 1))
            for k, start in enumerate((0, 30)):
                sums[k] = jnp.where(here, pltpu.roll(tile, (EDGE_LANES * i - start) % LANES, 1), sums[k])
            for k, ref in enumerate((o_ref, e_ref)):
                for s in range(3):
                    ref[3 * j + s] = r_ref[pl.ds(BLOCK * j + (0, 28)[k] + 8 * s, 8), :]
        o_ref[48 + g] = sums[0]
        e_ref[48 + g] = sums[1]


def side_beams(ref, steer_ref, beams_ref, halo_ref, side_ref):
    lane = lax.broadcasted_iota(jnp.int32, (8, LANES), 1)
    for j in range(16):
        tile = pltpu.roll(ref[48 + j // MERGED], -EDGE_LANES * (j % MERGED) % LANES, 1)
        halo_ref[j] = jnp.where(lane < EDGE_LANES, tile, 0.0)
    lines = ref[:48].reshape(16, 3, 8, LANES)
    for s in (0, 2):
        both = beam_pair(lines[:, s], lines[:, 1] if s == 0 else halo_ref[...], steer_ref, beams_ref)
        side_ref[s] = both[:, :LANES]
        side_ref[s + 1] = both[:, LANES:]


def beam_pair(first, second, steer_ref, beams_ref):
    both = jnp.concatenate([first.reshape(LANES, LANES), second.reshape(LANES, LANES)], axis=1)
    high = both.astype(jnp.bfloat16)
    low = (both - high.astype(jnp.float32)).astype(jnp.bfloat16)
    stacked = jnp.concatenate([high, low, high], axis=0)
    beams_ref[...] = jnp.dot(steer_ref[...], stacked, preferred_element_type=jnp.float32)
    re, im = beams_ref[:HEIGHTS], beams_ref[HEIGHTS:]
    power = re * re + im * im
    squares = (both * both).reshape(16, 8, 2 * LANES).sum(axis=0)
    return jnp.concatenate([power, squares], axis=0)


def own_kernel(r_ref, halo_ref, steer_ref, out_ref, beams_ref):
    def block(s):
        if s == HALO:
            return halo_ref[...]
        (m,) = [m for m in SLOT if SLOT[m] == s]
        return jnp.concatenate([r_ref[pl.ds(BLOCK * j + ROW[m], 8), :] for j in range(16)], axis=0)

    for s in (0, 2, 4, 6, 8):
        t = min(s + 1, 8)
        both = beam_pair(block(s), block(t), steer_ref, beams_ref)
        out_ref[s] = both[:, :LANES]
        if t != s:
            out_ref[t] = both[:, LANES:]


def halves(field):
    high = field.astype(jnp.bfloat16)
    low = (field - high.astype(jnp.float32)).astype(jnp.bfloat16)
    return jnp.concatenate([high, low], axis=1)


def boxed(total, correction):
    lane = lax.broadcasted_iota(jnp.int32, total.shape, 1)
    box = total + correction
    for d in (1, 2, 3):
        box = box + jnp.where(lane >= d, pltpu.roll(total, d, 1), 0.0)
        box = box + jnp.where(lane < LANES - d, pltpu.roll(total, LANES - d, 1), 0.0)
    return box


def normalize(m, odd, box_of, flat_ref):
    line = m + odd * (7 - 2 * m)
    energy = box_of(m, slice(HEIGHTS, ROWS)).sum(axis=0, keepdims=True)
    inverse = 1.0 / (energy + epsilon)
    for k in range(0, HEIGHTS, 64):
        flat_ref[pl.ds(8 * k + line, 64, stride=8), :] = box_of(m, slice(k, k + 64)) * inverse


def inner_kernel(own_ref, e_ref, steer_ref, mid_ref, me_ref, flat_ref, part_ref, cor_ref, beams_ref, halo_ref, side_ref, all_ref):
    side_beams(e_ref, steer_ref, beams_ref, halo_ref, side_ref)
    all_ref[...] = jnp.dot(halves(own_ref[HALO]), mid_ref[...], preferred_element_type=jnp.float32)
    all_ref[:, 5 * LANES :] += jnp.dot(halves(side_ref[3]), me_ref[...], preferred_element_type=jnp.float32)
    cor_ref[...] = all_ref[:, : 3 * LANES]

    def summed(m, rows):
        total = None
        for position in range(max(m - 3, 0), m + 4):
            term = side_ref[position - 8, rows] if position > 7 else own_ref[SLOT[position], rows]
            total = term if total is None else total + term
        return total

    for m in range(3):
        for k in range(0, ROWS, 88):
            part_ref[m, k : k + 88] = summed(m, slice(k, k + 88))
    odd = parity()
    for m in range(3, 8):
        normalize(m, odd, lambda m, rows: boxed(summed(m, rows), all_ref[rows, m * LANES : (m + 1) * LANES]), flat_ref)


def outer_kernel(o_ref, part_ref, cor_ref, flat_ref, steer_ref, mo_ref, out_ref, beams_ref, halo_ref, side_ref, all_ref, edge_ref, done_ref, sems):
    side_beams(o_ref, steer_ref, beams_ref, halo_ref, side_ref)
    all_ref[...] = cor_ref[...] + jnp.dot(halves(side_ref[3]), mo_ref[...], preferred_element_type=jnp.float32)

    def box_of(m, rows):
        total = part_ref[m, rows]
        for i in range(3 - m):
            total = total + side_ref[i, rows]
        return boxed(total, all_ref[rows, m * LANES : (m + 1) * LANES])

    odd = parity()
    for m in range(3):
        normalize(m, odd, box_of, edge_ref)
    sub = lax.broadcasted_iota(jnp.int32, (16, 8, LANES), 1)
    edge = jnp.where(odd == 1, 7 - sub, sub) < 3
    copies = []
    for q in range(4):
        for k in range(64 * q, 64 * q + 64, 16):
            rows = slice(8 * k, 8 * k + 128)
            merged = jnp.where(edge, edge_ref[rows].reshape(16, 8, LANES), flat_ref[rows].reshape(16, 8, LANES))
            done_ref[k : k + 16] = merged.astype(jnp.bfloat16)
        copy = pltpu.make_async_copy(done_ref.at[pl.ds(64 * q, 64)], out_ref.at[pl.ds(64 * q, 64)], sems.at[q])
        copy.start()
        copies.append(copy)
    for copy in copies:
        copy.wait()


def spread():
    column = np.array([-3, -2, -1, 128, 129, 130])
    near = np.abs(column[:, None] - np.arange(LANES)[None, :]) <= 3

    def matrix(position_of, lines, used, first=0):
        full = np.zeros((LANES, len(lines), LANES), np.float32)
        for n in used:
            for i, m in enumerate(lines):
                if abs(position_of(n) - m) <= 3:
                    full[6 * (n - first) : 6 * (n - first) + 6, i] = near
        full = full.reshape(LANES, -1)
        return jnp.asarray(np.concatenate([full, full], axis=0), jnp.bfloat16)

    mid = matrix(lambda n: n, range(8), range(8))
    mo = matrix(lambda n: -1 - n, (0, 1, 2), (0, 1, 2))
    me = matrix(lambda n: 15 - n, (5, 6, 7), (5, 6, 7), 5)
    return mid, mo, me


def steering(wavenumbers):
    source = np.array([4 * acq + k for acq in PLACE for _ in range(2) for k in range(4)])
    chosen = np.arange(len(source) // 2)[:, None] == source[None, :]
    waves = jnp.sum(jnp.where(chosen, wavenumbers[:, None], 0.0), axis=0)
    real = (np.arange(LANES) // 4) % 2 == 0
    heights = np.arange(HEIGHTS, dtype=np.float32) - np.float32(HEIGHTS // 2)
    phases = jnp.asarray(heights)[:, None] * waves[None, :]
    cosine, sine = jnp.cos(phases), jnp.sin(phases)
    full = jnp.concatenate([jnp.where(real, cosine, sine), jnp.where(real, -sine, cosine)], axis=0)
    high = lax.reduce_precision(full, 8, 7)
    low = (full - high).astype(jnp.bfloat16)
    high = high.astype(jnp.bfloat16)
    return jnp.concatenate([high, high, low], axis=1)


VMEM = pl.BlockSpec(memory_space=pltpu.VMEM)
ANY = pl.BlockSpec(memory_space=pl.ANY)


def call(kernel, shapes, vmem, flops, scratch=(), out=VMEM, dtype=jnp.float32):
    def on(*operands):
        return pl.pallas_call(
            kernel,
            out_shape=[jax.ShapeDtypeStruct(shape, dtype) for shape in shapes],
            in_specs=[VMEM] * len(operands),
            out_specs=[out] * len(shapes),
            scratch_shapes=list(scratch),
            compiler_params=pltpu.CompilerParams(vmem_limit_bytes=vmem << 20),
            cost_estimate=pl.CostEstimate(flops=flops, bytes_accessed=1000000, transcendentals=0),
        )(*operands)

    return on


def spectrum(slc_stack, wavenumbers):
    lines = lax.axis_size("line")
    outer = [pair for i in range(1, lines - 1, 2) for pair in ((i, i + 1), (i + 1, i))]
    inner = [pair for i in range(0, lines, 2) for pair in ((i, i + 1), (i + 1, i))]
    beams = pltpu.VMEM((2 * HEIGHTS, 2 * LANES), jnp.float32)
    strip = pltpu.VMEM((16, 8, LANES), jnp.float32)
    quad = pltpu.VMEM((4, ROWS, LANES), jnp.float32)
    stack = slc_stack.reshape(8, 8, -1, LANES).transpose(0, 2, 1, 3).reshape(-1, LANES)
    (packed,) = call(pack_kernel, [(16 * BLOCK, LANES)], 2, 1000000)(stack)
    packed = packed.reshape(16, BLOCK, 1, LANES)
    gathered = lax.all_to_all(packed, "acq", 0, 0, tiled=True, axis_index_groups=[PLACE])
    gathered = gathered.reshape(16 * BLOCK, LANES)
    sides = (EDGE_TILES, 8, LANES)
    to_o, to_e, halo = call(edge_kernel, [sides, sides, (16, 8, LANES)], 4, 1000000)(gathered)
    mid, mo, me = spread()
    to_o, to_e, wavenumbers = lax.optimization_barrier((to_o, to_e, wavenumbers))
    steer = steering(wavenumbers)
    side_o = lax.ppermute(to_o, "line", outer)
    side_e = lax.ppermute(to_e, "line", inner)
    (own,) = call(own_kernel, [(9, ROWS, LANES)], 10, 1000000000, [beams])(gathered, halo, steer)
    flat, part, cor = call(
        inner_kernel,
        [(8 * HEIGHTS, LANES), (3, ROWS, LANES), (ROWS, 3 * LANES)],
        14,
        1000000000,
        [beams, strip, quad, pltpu.VMEM((ROWS, 8 * LANES), jnp.float32)],
    )(own, side_e, steer, mid, me)
    (result,) = call(
        outer_kernel,
        [(HEIGHTS, 8, LANES)],
        12,
        1000000000,
        [
            beams,
            strip,
            quad,
            pltpu.VMEM((ROWS, 3 * LANES), jnp.float32),
            pltpu.VMEM((8 * HEIGHTS, LANES), jnp.float32),
            pltpu.VMEM((HEIGHTS, 8, LANES), jnp.bfloat16),
            pltpu.SemaphoreType.DMA((4,)),
        ],
        out=ANY,
        dtype=jnp.bfloat16,
    )(side_o, part, cor, flat, steer, mo)
    return result


def solution(mesh):
    placed = (P(None, "acq", "line", None), P())
    return jax.shard_map(spectrum, mesh=mesh, in_specs=placed, out_specs=P(None, "line", "acq"), check_vma=False)
```

```python
import jax
import jax.numpy as jnp
import numpy as np
from jax import lax
from jax.experimental import pallas as pl
from jax.experimental.pallas import tpu as pltpu
from jax.sharding import PartitionSpec as P


HEIGHTS = 256
ROWS = HEIGHTS + 8
LANES = 128
epsilon = 1e-06

ROW = {0: 0, 1: 8, 2: 16, 7: 28, 6: 36, 5: 44, 3: 52, 4: 60}
HALO_ROW = 24
BLOCK = 68
HELD = (16, 12)
SLOT = {0: 0, 1: 1, 2: 2, 7: 4, 6: 5, 5: 6, 3: 7, 4: 8}
HALO = 3
EDGE_LANES = 18
MERGED = 7
EDGE_TILES = 48 + 3
PLACE = [2 * z + y for z in (4, 3, 5, 2, 6, 1, 7, 0) for y in (0, 1)]


def parity():
    return lax.rem(lax.axis_index("line"), 2)


def pack(x_ref, out_ref):
    blocks = x_ref.shape[0] // 64
    odd = parity()
    lane = lax.broadcasted_iota(jnp.int32, (8, LANES), 1)
    zero = jnp.zeros((8, LANES), jnp.float32)
    halo = [zero, zero]
    for j in range(blocks):
        halo.append(zero)
        for m in range(8):
            line = m + odd * (7 - 2 * m)
            tile = x_ref[pl.ds(8 * j + line, 8, stride=8 * blocks), :]
            out_ref[pl.ds(BLOCK * PLACE.index(j) + ROW[m], 8), :] = tile
            left = (lane >= 6 * m) & (lane < 6 * m + 3)
            right = (lane >= 6 * m + 3) & (lane < 6 * m + 6)
            moved = pltpu.roll(tile, 6 * m + 3, 1)
            halo[j + 2] = jnp.where(left, moved, halo[j + 2])
            halo[j] = jnp.where(right, moved, halo[j])
    for j in range(blocks):
        tile = halo[j + 1]
        tile = tile + pltpu.roll(pltpu.roll(tile, 4, 0), LANES // 2, 1)
        out_ref[pl.ds(BLOCK * PLACE.index(j) + HALO_ROW, 4), :] = tile[:4]


def pack_kernel(x_ref, out_ref):
    row = lax.rem(lax.axis_index("line"), 8)
    times = 1 + jnp.where(row == 1, HELD[0], jnp.where(row == 6, HELD[1], 0))

    def once(_, carry):
        pack(x_ref, out_ref)
        return carry

    lax.fori_loop(0, times, once, 0)


def edge_kernel(r_ref, o_ref, e_ref, halo_ref):
    lane = lax.broadcasted_iota(jnp.int32, (8, LANES), 1)
    sub = lax.broadcasted_iota(jnp.int32, (8, LANES), 0)
    for g in range(3):
        sums = [jnp.zeros((8, LANES), jnp.float32) for _ in range(2)]
        for i in range(min(MERGED, 16 - MERGED * g)):
            j = MERGED * g + i
            tile = r_ref[pl.ds(BLOCK * j + HALO_ROW, 8), :]
            tile = jnp.where(sub < 4, tile, pltpu.roll(pltpu.roll(tile, 4, 0), LANES // 2, 1))
            tile = jnp.where(lane < 48, tile, 0.0)
            halo_ref[j] = tile
            here = (lane >= EDGE_LANES * i) & (lane < EDGE_LANES * (i + 1))
            for k, start in enumerate((0, 30)):
                sums[k] = jnp.where(here, pltpu.roll(tile, (EDGE_LANES * i - start) % LANES, 1), sums[k])
            for k, ref in enumerate((o_ref, e_ref)):
                for s in range(3):
                    ref[3 * j + s] = r_ref[pl.ds(BLOCK * j + (0, 28)[k] + 8 * s, 8), :]
        o_ref[48 + g] = sums[0]
        e_ref[48 + g] = sums[1]


def side_beams(ref, steer_ref, beams_ref, halo_ref, side_ref):
    lane = lax.broadcasted_iota(jnp.int32, (8, LANES), 1)
    for j in range(16):
        tile = pltpu.roll(ref[48 + j // MERGED], -EDGE_LANES * (j % MERGED) % LANES, 1)
        halo_ref[j] = jnp.where(lane < EDGE_LANES, tile, 0.0)
    lines = ref[:48].reshape(16, 3, 8, LANES)
    for s in (0, 2):
        both = beam_pair(lines[:, s], lines[:, 1] if s == 0 else halo_ref[...], steer_ref, beams_ref)
        side_ref[s] = both[:, :LANES]
        side_ref[s + 1] = both[:, LANES:]


def beam_pair(first, second, steer_ref, beams_ref):
    both = jnp.concatenate([first.reshape(LANES, LANES), second.reshape(LANES, LANES)], axis=1)
    high = both.astype(jnp.bfloat16)
    low = (both - high.astype(jnp.float32)).astype(jnp.bfloat16)
    stacked = jnp.concatenate([high, low, high], axis=0)
    beams_ref[...] = jnp.dot(steer_ref[...], stacked, preferred_element_type=jnp.float32)
    re, im = beams_ref[:HEIGHTS], beams_ref[HEIGHTS:]
    power = re * re + im * im
    squares = (both * both).reshape(16, 8, 2 * LANES).sum(axis=0)
    return jnp.concatenate([power, squares], axis=0)


def own_kernel(r_ref, halo_ref, steer_ref, out_ref, beams_ref):
    def block(s):
        if s == HALO:
            return halo_ref[...]
        (m,) = [m for m in SLOT if SLOT[m] == s]
        return jnp.concatenate([r_ref[pl.ds(BLOCK * j + ROW[m], 8), :] for j in range(16)], axis=0)

    for s in (0, 2, 4, 6, 8):
        t = min(s + 1, 8)
        both = beam_pair(block(s), block(t), steer_ref, beams_ref)
        out_ref[s] = both[:, :LANES]
        if t != s:
            out_ref[t] = both[:, LANES:]


def halves(field):
    high = field.astype(jnp.bfloat16)
    low = (field - high.astype(jnp.float32)).astype(jnp.bfloat16)
    return jnp.concatenate([high, low], axis=1)


def boxed(total, correction):
    lane = lax.broadcasted_iota(jnp.int32, total.shape, 1)
    box = total + correction
    for d in (1, 2, 3):
        box = box + jnp.where(lane >= d, pltpu.roll(total, d, 1), 0.0)
        box = box + jnp.where(lane < LANES - d, pltpu.roll(total, LANES - d, 1), 0.0)
    return box


def normalize(m, odd, box_of, flat_ref):
    line = m + odd * (7 - 2 * m)
    energy = box_of(m, slice(HEIGHTS, ROWS)).sum(axis=0, keepdims=True)
    inverse = 1.0 / (energy + epsilon)
    for k in range(0, HEIGHTS, 64):
        flat_ref[pl.ds(8 * k + line, 64, stride=8), :] = box_of(m, slice(k, k + 64)) * inverse


def inner_kernel(own_ref, e_ref, steer_ref, mid_ref, me_ref, flat_ref, part_ref, cor_ref, beams_ref, halo_ref, side_ref, all_ref):
    side_beams(e_ref, steer_ref, beams_ref, halo_ref, side_ref)
    all_ref[...] = jnp.dot(halves(own_ref[HALO]), mid_ref[...], preferred_element_type=jnp.float32)
    all_ref[:, 5 * LANES :] += jnp.dot(halves(side_ref[3]), me_ref[...], preferred_element_type=jnp.float32)
    cor_ref[...] = all_ref[:, : 3 * LANES]

    def summed(m, rows):
        total = None
        for position in range(max(m - 3, 0), m + 4):
            term = side_ref[position - 8, rows] if position > 7 else own_ref[SLOT[position], rows]
            total = term if total is None else total + term
        return total

    for m in range(3):
        for k in range(0, ROWS, 88):
            part_ref[m, k : k + 88] = summed(m, slice(k, k + 88))
    odd = parity()
    for m in range(3, 8):
        normalize(m, odd, lambda m, rows: boxed(summed(m, rows), all_ref[rows, m * LANES : (m + 1) * LANES]), flat_ref)


def outer_kernel(o_ref, part_ref, cor_ref, flat_ref, steer_ref, mo_ref, out_ref, beams_ref, halo_ref, side_ref, all_ref, edge_ref, done_ref, sems):
    side_beams(o_ref, steer_ref, beams_ref, halo_ref, side_ref)
    all_ref[...] = cor_ref[...] + jnp.dot(halves(side_ref[3]), mo_ref[...], preferred_element_type=jnp.float32)

    def box_of(m, rows):
        total = part_ref[m, rows]
        for i in range(3 - m):
            total = total + side_ref[i, rows]
        return boxed(total, all_ref[rows, m * LANES : (m + 1) * LANES])

    odd = parity()
    for m in range(3):
        normalize(m, odd, box_of, edge_ref)
    sub = lax.broadcasted_iota(jnp.int32, (16, 8, LANES), 1)
    edge = jnp.where(odd == 1, 7 - sub, sub) < 3
    copies = []
    for q in range(4):
        for k in range(64 * q, 64 * q + 64, 16):
            rows = slice(8 * k, 8 * k + 128)
            merged = jnp.where(edge, edge_ref[rows].reshape(16, 8, LANES), flat_ref[rows].reshape(16, 8, LANES))
            done_ref[k : k + 16] = merged.astype(jnp.bfloat16)
        copy = pltpu.make_async_copy(done_ref.at[pl.ds(64 * q, 64)], out_ref.at[pl.ds(64 * q, 64)], sems.at[q])
        copy.start()
        copies.append(copy)
    for copy in copies:
        copy.wait()


def spread():
    column = np.array([-3, -2, -1, 128, 129, 130])
    near = np.abs(column[:, None] - np.arange(LANES)[None, :]) <= 3

    def matrix(position_of, lines, used, first=0):
        full = np.zeros((LANES, len(lines), LANES), np.float32)
        for n in used:
            for i, m in enumerate(lines):
                if abs(position_of(n) - m) <= 3:
                    full[6 * (n - first) : 6 * (n - first) + 6, i] = near
        full = full.reshape(LANES, -1)
        return jnp.asarray(np.concatenate([full, full], axis=0), jnp.bfloat16)

    mid = matrix(lambda n: n, range(8), range(8))
    mo = matrix(lambda n: -1 - n, (0, 1, 2), (0, 1, 2))
    me = matrix(lambda n: 15 - n, (5, 6, 7), (5, 6, 7), 5)
    return mid, mo, me


def steering(wavenumbers):
    source = np.array([4 * acq + k for acq in PLACE for _ in range(2) for k in range(4)])
    chosen = np.arange(len(source) // 2)[:, None] == source[None, :]
    waves = jnp.sum(jnp.where(chosen, wavenumbers[:, None], 0.0), axis=0)
    real = (np.arange(LANES) // 4) % 2 == 0
    heights = np.arange(HEIGHTS, dtype=np.float32) - np.float32(HEIGHTS // 2)
    phases = jnp.asarray(heights)[:, None] * waves[None, :]
    cosine, sine = jnp.cos(phases), jnp.sin(phases)
    full = jnp.concatenate([jnp.where(real, cosine, sine), jnp.where(real, -sine, cosine)], axis=0)
    high = lax.reduce_precision(full, 8, 7)
    low = (full - high).astype(jnp.bfloat16)
    high = high.astype(jnp.bfloat16)
    return jnp.concatenate([high, high, low], axis=1)


VMEM = pl.BlockSpec(memory_space=pltpu.VMEM)
ANY = pl.BlockSpec(memory_space=pl.ANY)


def call(kernel, shapes, vmem, flops, scratch=(), out=VMEM, dtype=jnp.float32):
    def on(*operands):
        return pl.pallas_call(
            kernel,
            out_shape=[jax.ShapeDtypeStruct(shape, dtype) for shape in shapes],
            in_specs=[VMEM] * len(operands),
            out_specs=[out] * len(shapes),
            scratch_shapes=list(scratch),
            compiler_params=pltpu.CompilerParams(vmem_limit_bytes=vmem << 20),
            cost_estimate=pl.CostEstimate(flops=flops, bytes_accessed=1000000, transcendentals=0),
        )(*operands)

    return on


def spectrum(slc_stack, wavenumbers):
    lines = lax.axis_size("line")
    outer = [pair for i in range(1, lines - 1, 2) for pair in ((i, i + 1), (i + 1, i))]
    inner = [pair for i in range(0, lines, 2) for pair in ((i, i + 1), (i + 1, i))]
    beams = pltpu.VMEM((2 * HEIGHTS, 2 * LANES), jnp.float32)
    strip = pltpu.VMEM((16, 8, LANES), jnp.float32)
    quad = pltpu.VMEM((4, ROWS, LANES), jnp.float32)
    stack = slc_stack.reshape(8, 8, -1, LANES).transpose(0, 2, 1, 3).reshape(-1, LANES)
    (packed,) = call(pack_kernel, [(16 * BLOCK, LANES)], 2, 1000000)(stack)
    packed = packed.reshape(16, BLOCK, 1, LANES)
    gathered = lax.all_to_all(packed, "acq", 0, 0, tiled=True, axis_index_groups=[PLACE])
    gathered = gathered.reshape(16 * BLOCK, LANES)
    sides = (EDGE_TILES, 8, LANES)
    to_o, to_e, halo = call(edge_kernel, [sides, sides, (16, 8, LANES)], 4, 1000000)(gathered)
    mid, mo, me = spread()
    to_o, to_e, wavenumbers = lax.optimization_barrier((to_o, to_e, wavenumbers))
    steer = steering(wavenumbers)
    side_o = lax.ppermute(to_o, "line", outer)
    side_e = lax.ppermute(to_e, "line", inner)
    (own,) = call(own_kernel, [(9, ROWS, LANES)], 10, 1000000000, [beams])(gathered, halo, steer)
    flat, part, cor = call(
        inner_kernel,
        [(8 * HEIGHTS, LANES), (3, ROWS, LANES), (ROWS, 3 * LANES)],
        14,
        1000000000,
        [beams, strip, quad, pltpu.VMEM((ROWS, 8 * LANES), jnp.float32)],
    )(own, side_e, steer, mid, me)
    (result,) = call(
        outer_kernel,
        [(HEIGHTS, 8, LANES)],
        12,
        1000000000,
        [
            beams,
            strip,
            quad,
            pltpu.VMEM((ROWS, 3 * LANES), jnp.float32),
            pltpu.VMEM((8 * HEIGHTS, LANES), jnp.float32),
            pltpu.VMEM((HEIGHTS, 8, LANES), jnp.bfloat16),
            pltpu.SemaphoreType.DMA((4,)),
        ],
        out=ANY,
        dtype=jnp.bfloat16,
    )(side_o, part, cor, flat, steer, mo)
    return result


def solution(mesh):
    placed = (P(None, "acq", "line", None), P())
    return jax.shard_map(spectrum, mesh=mesh, in_specs=placed, out_specs=P(None, "line", "acq"), check_vma=False)
```

```python
import jax
import jax.numpy as jnp
import numpy as np
from jax import lax
from jax.experimental import pallas as pl
from jax.experimental.pallas import tpu as pltpu
from jax.sharding import PartitionSpec as P


HEIGHTS = 256
ROWS = HEIGHTS + 8
LANES = 128
epsilon = 1e-06

ROW = {0: 0, 1: 8, 2: 16, 7: 28, 6: 36, 5: 44, 3: 52, 4: 60}
HALO_ROW = 24
BLOCK = 68
HELD = (26, 17)
SLOT = {0: 0, 1: 1, 2: 2, 7: 4, 6: 5, 5: 6, 3: 7, 4: 8}
HALO = 3
EDGE_LANES = 18
MERGED = 7
EDGE_TILES = 48 + 3
PLACE = [2 * z + y for z in (4, 3, 5, 2, 6, 1, 7, 0) for y in (0, 1)]


def parity():
    return lax.rem(lax.axis_index("line"), 2)


def transposed(tiles):
    sub = lax.broadcasted_iota(jnp.int32, (8, LANES), 0)
    tiles = list(tiles)
    for d in (4, 2, 1):
        low = (sub & d) == 0
        for i in range(8):
            if i & d == 0:
                a, b = tiles[i], tiles[i + d]
                tiles[i] = jnp.where(low, a, pltpu.roll(b, d, 0))
                tiles[i + d] = jnp.where(low, pltpu.roll(a, 8 - d, 0), b)
    return tiles


def turned(tiles, odd):
    return [jnp.where(odd, tiles[-1 - i], tile) for i, tile in enumerate(tiles)]


def pack(x_ref, out_ref):
    blocks = x_ref.shape[0] // 64
    odd = parity() == 1
    lane = lax.broadcasted_iota(jnp.int32, (8, LANES), 1)
    zero = jnp.zeros((8, LANES), jnp.float32)
    halo = [zero, zero]
    for j in range(blocks):
        halo.append(zero)
        rows = [slice(8 * (blocks * channel + j), 8 * (blocks * channel + j) + 8) for channel in range(8)]
        for m, tile in enumerate(turned(transposed([x_ref[r] for r in rows]), odd)):
            out_ref[pl.ds(BLOCK * PLACE.index(j) + ROW[m], 8), :] = tile
            left = (lane >= 6 * m) & (lane < 6 * m + 3)
            right = (lane >= 6 * m + 3) & (lane < 6 * m + 6)
            moved = pltpu.roll(tile, 6 * m + 3, 1)
            halo[j + 2] = jnp.where(left, moved, halo[j + 2])
            halo[j] = jnp.where(right, moved, halo[j])
    for j in range(blocks):
        tile = halo[j + 1]
        tile = tile + pltpu.roll(pltpu.roll(tile, 4, 0), LANES // 2, 1)
        out_ref[pl.ds(BLOCK * PLACE.index(j) + HALO_ROW, 4), :] = tile[:4]


def pack_kernel(x_ref, out_ref):
    line, lines = lax.axis_index("line"), lax.axis_size("line")
    row = lax.rem(line, 8)
    first, last = (row == 1) & (line > 1), (row == 6) & (line < lines - 2)
    times = 1 + jnp.where(first, HELD[0], jnp.where(last, HELD[1], 0))

    def once(_, carry):
        pack(x_ref, out_ref)
        return carry

    lax.fori_loop(0, times, once, 0)


def edge_kernel(r_ref, o_ref, e_ref, halo_ref):
    lane = lax.broadcasted_iota(jnp.int32, (8, LANES), 1)
    sub = lax.broadcasted_iota(jnp.int32, (8, LANES), 0)
    for g in range(3):
        sums = [jnp.zeros((8, LANES), jnp.float32) for _ in range(2)]
        for i in range(min(MERGED, 16 - MERGED * g)):
            j = MERGED * g + i
            tile = r_ref[pl.ds(BLOCK * j + HALO_ROW, 8), :]
            tile = jnp.where(sub < 4, tile, pltpu.roll(pltpu.roll(tile, 4, 0), LANES // 2, 1))
            tile = jnp.where(lane < 48, tile, 0.0)
            halo_ref[j] = tile
            here = (lane >= EDGE_LANES * i) & (lane < EDGE_LANES * (i + 1))
            for k, start in enumerate((0, 30)):
                sums[k] = jnp.where(here, pltpu.roll(tile, (EDGE_LANES * i - start) % LANES, 1), sums[k])
            for k, ref in enumerate((o_ref, e_ref)):
                for s in range(3):
                    ref[3 * j + s] = r_ref[pl.ds(BLOCK * j + (0, 28)[k] + 8 * s, 8), :]
        o_ref[48 + g] = sums[0]
        e_ref[48 + g] = sums[1]


def side_beams(ref, steer_ref, halo_ref, side_ref):
    lane = lax.broadcasted_iota(jnp.int32, (8, LANES), 1)
    for j in range(16):
        tile = pltpu.roll(ref[48 + j // MERGED], -EDGE_LANES * (j % MERGED) % LANES, 1)
        halo_ref[j] = jnp.where(lane < EDGE_LANES, tile, 0.0)
    lines = ref[:48].reshape(16, 3, 8, LANES)
    for s in (0, 2):
        both = beam_pair(lines[:, s], lines[:, 1] if s == 0 else halo_ref[...], steer_ref)
        side_ref[s] = both[:, :LANES]
        side_ref[s + 1] = both[:, LANES:]


def beam_pair(first, second, steer_ref):
    both = jnp.concatenate([first.reshape(LANES, LANES), second.reshape(LANES, LANES)], axis=1)
    high = both.astype(jnp.bfloat16)
    low = (both - high.astype(jnp.float32)).astype(jnp.bfloat16)
    stacked = jnp.concatenate([high, low, high], axis=0)
    beams = jnp.dot(steer_ref[...], stacked, preferred_element_type=jnp.float32)
    beams = beams.reshape(HEIGHTS // 8, 2, 8, 2 * LANES)
    power = beams[:, 0] * beams[:, 0] + beams[:, 1] * beams[:, 1]
    squares = (both * both).reshape(16, 8, 2 * LANES).sum(axis=0)
    return jnp.concatenate([power.reshape(HEIGHTS, 2 * LANES), squares], axis=0)


def own_kernel(r_ref, halo_ref, steer_ref, out_ref):
    def block(s):
        if s == HALO:
            return halo_ref[...]
        (m,) = [m for m in SLOT if SLOT[m] == s]
        return jnp.concatenate([r_ref[pl.ds(BLOCK * j + ROW[m], 8), :] for j in range(16)], axis=0)

    for s in (0, 2, 4, 6, 8):
        t = min(s + 1, 8)
        both = beam_pair(block(s), block(t), steer_ref)
        out_ref[s] = both[:, :LANES]
        if t != s:
            out_ref[t] = both[:, LANES:]


def halves(field):
    high = field.astype(jnp.bfloat16)
    low = (field - high.astype(jnp.float32)).astype(jnp.bfloat16)
    return jnp.concatenate([high, low], axis=1)


def boxed(total, correction, few):
    lane = lax.broadcasted_iota(jnp.int32, total.shape, 1)

    def after(field, d):
        return jnp.where(lane >= d, pltpu.roll(field, d, 1), 0.0)

    def before(field, d):
        return jnp.where(lane < LANES - d, pltpu.roll(field, LANES - d, 1), 0.0)

    if few:
        right, left = total + after(total, 1), before(total, 1)
        return (right + after(right, 2)) + (left + before(total + left, 2)) + correction
    box = total + correction
    for d in (1, 2, 3):
        box = (box + after(total, d)) + before(total, d)
    return box


def normalize(box_of, ref):
    inverse = [1.0 / (box.sum(axis=0, keepdims=True) + epsilon) for box in box_of(slice(HEIGHTS, ROWS))]
    for k in range(0, HEIGHTS, 8):
        for n, box in enumerate(box_of(slice(k, k + 8))):
            ref[n, k : k + 8] = box * inverse[n]


def inner_kernel(own_ref, e_ref, steer_ref, mid_ref, me_ref, done_ref, part_ref, cor_ref, halo_ref, side_ref, all_ref):
    side_beams(e_ref, steer_ref, halo_ref, side_ref)
    all_ref[...] = jnp.dot(halves(own_ref[HALO]), mid_ref[...], preferred_element_type=jnp.float32)
    all_ref[:, 5 * LANES :] += jnp.dot(halves(side_ref[3]), me_ref[...], preferred_element_type=jnp.float32)
    cor_ref[...] = all_ref[:, : 3 * LANES]

    def box_of(rows):
        ones = [own_ref[SLOT[m], rows] for m in range(8)] + [side_ref[n, rows] for n in range(3)]
        twos = [a + b for a, b in zip(ones[:-1], ones[1:])]
        fours = [a + b for a, b in zip(twos[:-2], twos[2:])]
        for m, total in enumerate((fours[0], fours[0] + ones[4], fours[0] + twos[4])):
            part_ref[m, rows] = total
        sums = [fours[n] + (twos[n + 4] + ones[n + 6]) for n in range(5)]
        return [boxed(total, all_ref[rows, (n + 3) * LANES : (n + 4) * LANES], False) for n, total in enumerate(sums)]

    normalize(box_of, done_ref)


def outer_kernel(o_ref, part_ref, cor_ref, lines_ref, steer_ref, mo_ref, out_ref, halo_ref, side_ref, all_ref, edge_ref, done_ref, sems):
    side_beams(o_ref, steer_ref, halo_ref, side_ref)
    all_ref[...] = cor_ref[...] + jnp.dot(halves(side_ref[3]), mo_ref[...], preferred_element_type=jnp.float32)

    def box_of(rows):
        near, next_, far = (side_ref[n, rows] for n in range(3))
        two = near + next_
        sums = (part_ref[0, rows] + (two + far), part_ref[1, rows] + two, part_ref[2, rows] + near)
        return [boxed(total, all_ref[rows, n * LANES : (n + 1) * LANES], True) for n, total in enumerate(sums)]

    normalize(box_of, edge_ref)
    odd = parity() == 1
    copies = []
    for q in range(4):
        for k in range(64 * q, 64 * q + 64, 8):
            tiles = [edge_ref[m, k : k + 8] for m in range(3)] + [lines_ref[m, k : k + 8] for m in range(5)]
            done_ref[k : k + 8] = jnp.stack(transposed(turned(tiles, odd))).astype(jnp.bfloat16)
        copy = pltpu.make_async_copy(done_ref.at[pl.ds(64 * q, 64)], out_ref.at[pl.ds(64 * q, 64)], sems.at[q])
        copy.start()
        copies.append(copy)
    for copy in copies:
        copy.wait()


def spread():
    column = np.array([-3, -2, -1, 128, 129, 130])
    near = np.abs(column[:, None] - np.arange(LANES)[None, :]) <= 3

    def matrix(position_of, lines, used, first=0):
        full = np.zeros((LANES, len(lines), LANES), np.float32)
        for n in used:
            for i, m in enumerate(lines):
                if abs(position_of(n) - m) <= 3:
                    full[6 * (n - first) : 6 * (n - first) + 6, i] = near
        full = full.reshape(LANES, -1)
        return jnp.asarray(np.concatenate([full, full], axis=0), jnp.bfloat16)

    mid = matrix(lambda n: n, range(8), range(8))
    mo = matrix(lambda n: -1 - n, (0, 1, 2), (0, 1, 2))
    me = matrix(lambda n: 15 - n, (5, 6, 7), (5, 6, 7), 5)
    return mid, mo, me


def steering(wavenumbers):
    source = np.array([4 * acq + k for acq in PLACE for _ in range(2) for k in range(4)])
    chosen = np.arange(len(source) // 2)[:, None] == source[None, :]
    waves = jnp.sum(jnp.where(chosen, wavenumbers[:, None], 0.0), axis=0)
    real = (np.arange(LANES) // 4) % 2 == 0
    heights = np.arange(HEIGHTS, dtype=np.float32) - np.float32(HEIGHTS // 2)
    phases = jnp.asarray(heights)[:, None] * waves[None, :]
    cosine, sine = jnp.cos(phases), jnp.sin(phases)
    full = jnp.concatenate([jnp.where(real, cosine, sine), jnp.where(real, -sine, cosine)], axis=0)
    full = full.reshape(2, HEIGHTS // 8, 8, LANES).transpose(1, 0, 2, 3).reshape(2 * HEIGHTS, LANES)
    high = lax.reduce_precision(full, 8, 7)
    low = (full - high).astype(jnp.bfloat16)
    high = high.astype(jnp.bfloat16)
    return jnp.concatenate([high, high, low], axis=1)


VMEM = pl.BlockSpec(memory_space=pltpu.VMEM)
ANY = pl.BlockSpec(memory_space=pl.ANY)


def call(kernel, shapes, vmem, flops, scratch=(), out=VMEM, dtype=jnp.float32):
    def on(*operands):
        return pl.pallas_call(
            kernel,
            out_shape=[jax.ShapeDtypeStruct(shape, dtype) for shape in shapes],
            in_specs=[VMEM] * len(operands),
            out_specs=[out] * len(shapes),
            scratch_shapes=list(scratch),
            compiler_params=pltpu.CompilerParams(vmem_limit_bytes=vmem << 20),
            cost_estimate=pl.CostEstimate(flops=flops, bytes_accessed=1000000, transcendentals=0),
        )(*operands)

    return on


def spectrum(slc_stack, wavenumbers):
    lines = lax.axis_size("line")
    outer = [pair for i in range(1, lines - 1, 2) for pair in ((i, i + 1), (i + 1, i))]
    inner = [pair for i in range(0, lines, 2) for pair in ((i, i + 1), (i + 1, i))]
    strip = pltpu.VMEM((16, 8, LANES), jnp.float32)
    quad = pltpu.VMEM((4, ROWS, LANES), jnp.float32)
    stack = slc_stack.reshape(8, 8, -1, LANES).transpose(0, 2, 1, 3).reshape(-1, LANES)
    (packed,) = call(pack_kernel, [(16 * BLOCK, LANES)], 2, 1000000)(stack)
    packed = packed.reshape(16, BLOCK, 1, LANES)
    gathered = lax.all_to_all(packed, "acq", 0, 0, tiled=True, axis_index_groups=[PLACE])
    gathered = gathered.reshape(16 * BLOCK, LANES)
    sides = (EDGE_TILES, 8, LANES)
    to_o, to_e, halo = call(edge_kernel, [sides, sides, (16, 8, LANES)], 4, 1000000)(gathered)
    mid, mo, me = spread()
    to_o, to_e, wavenumbers = lax.optimization_barrier((to_o, to_e, wavenumbers))
    steer = steering(wavenumbers)
    side_o = lax.ppermute(to_o, "line", outer)
    side_e = lax.ppermute(to_e, "line", inner)
    (own,) = call(own_kernel, [(9, ROWS, LANES)], 10, 1000000000)(gathered, halo, steer)
    rest, part, cor = call(
        inner_kernel,
        [(5, HEIGHTS, LANES), (3, ROWS, LANES), (ROWS, 3 * LANES)],
        14,
        1000000000,
        [strip, quad, pltpu.VMEM((ROWS, 8 * LANES), jnp.float32)],
    )(own, side_e, steer, mid, me)
    (result,) = call(
        outer_kernel,
        [(HEIGHTS, 8, LANES)],
        12,
        1000000000,
        [
            strip,
            quad,
            pltpu.VMEM((ROWS, 3 * LANES), jnp.float32),
            pltpu.VMEM((3, HEIGHTS, LANES), jnp.float32),
            pltpu.VMEM((HEIGHTS, 8, LANES), jnp.bfloat16),
            pltpu.SemaphoreType.DMA((4,)),
        ],
        out=ANY,
        dtype=jnp.bfloat16,
    )(side_o, part, cor, rest, steer, mo)
    return result


def solution(mesh):
    placed = (P(None, "acq", "line", None), P())
    return jax.shard_map(spectrum, mesh=mesh, in_specs=placed, out_specs=P(None, "line", "acq"), check_vma=False)
```

```python
import jax
import jax.numpy as jnp
import numpy as np
from jax import lax
from jax.experimental import pallas as pl
from jax.experimental.pallas import tpu as pltpu
from jax.sharding import PartitionSpec as P


HEIGHTS = 256
ROWS = HEIGHTS + 8
LANES = 128
epsilon = 1e-06

ROW = {0: 0, 1: 8, 2: 16, 7: 28, 6: 36, 5: 44, 3: 52, 4: 60}
HALO_ROW = 24
BLOCK = 68
HELD = (26, 17)
SLOT = {0: 0, 1: 1, 2: 2, 7: 4, 6: 5, 5: 6, 3: 7, 4: 8}
HALO = 3
EDGE_LANES = 18
MERGED = 7
EDGE_TILES = 48 + 3
PLACE = [2 * z + y for z in (4, 3, 5, 2, 6, 1, 7, 0) for y in (0, 1)]


def parity():
    return lax.rem(lax.axis_index("line"), 2)


def transposed(tiles):
    sub = lax.broadcasted_iota(jnp.int32, (8, LANES), 0)
    tiles = list(tiles)
    for d in (4, 2, 1):
        low = (sub & d) == 0
        for i in range(8):
            if i & d == 0:
                a, b = tiles[i], tiles[i + d]
                tiles[i] = jnp.where(low, a, pltpu.roll(b, d, 0))
                tiles[i + d] = jnp.where(low, pltpu.roll(a, 8 - d, 0), b)
    return tiles


def turned(tiles, odd):
    return [jnp.where(odd, tiles[-1 - i], tile) for i, tile in enumerate(tiles)]


def pack(x_ref, out_ref):
    blocks = x_ref.shape[0] // 64
    odd = parity() == 1
    lane = lax.broadcasted_iota(jnp.int32, (8, LANES), 1)
    zero = jnp.zeros((8, LANES), jnp.float32)
    halo = [zero, zero]
    for j in range(blocks):
        halo.append(zero)
        rows = [slice(8 * (blocks * channel + j), 8 * (blocks * channel + j) + 8) for channel in range(8)]
        for m, tile in enumerate(turned(transposed([x_ref[r] for r in rows]), odd)):
            out_ref[pl.ds(BLOCK * PLACE.index(j) + ROW[m], 8), :] = tile
            left = (lane >= 6 * m) & (lane < 6 * m + 3)
            right = (lane >= 6 * m + 3) & (lane < 6 * m + 6)
            moved = pltpu.roll(tile, 6 * m + 3, 1)
            halo[j + 2] = jnp.where(left, moved, halo[j + 2])
            halo[j] = jnp.where(right, moved, halo[j])
    for j in range(blocks):
        tile = halo[j + 1]
        tile = tile + pltpu.roll(pltpu.roll(tile, 4, 0), LANES // 2, 1)
        out_ref[pl.ds(BLOCK * PLACE.index(j) + HALO_ROW, 4), :] = tile[:4]


def pack_kernel(x_ref, out_ref):
    line, lines = lax.axis_index("line"), lax.axis_size("line")
    row = lax.rem(line, 8)
    first, last = (row == 1) & (line > 1), (row == 6) & (line < lines - 2)
    times = 1 + jnp.where(first, HELD[0], jnp.where(last, HELD[1], 0))

    def once(_, carry):
        pack(x_ref, out_ref)
        return carry

    lax.fori_loop(0, times, once, 0)


def edge_kernel(r_ref, o_ref, e_ref, halo_ref):
    lane = lax.broadcasted_iota(jnp.int32, (8, LANES), 1)
    sub = lax.broadcasted_iota(jnp.int32, (8, LANES), 0)
    for g in range(3):
        sums = [jnp.zeros((8, LANES), jnp.float32) for _ in range(2)]
        for i in range(min(MERGED, 16 - MERGED * g)):
            j = MERGED * g + i
            tile = r_ref[pl.ds(BLOCK * j + HALO_ROW, 8), :]
            tile = jnp.where(sub < 4, tile, pltpu.roll(pltpu.roll(tile, 4, 0), LANES // 2, 1))
            tile = jnp.where(lane < 48, tile, 0.0)
            halo_ref[j] = tile
            here = (lane >= EDGE_LANES * i) & (lane < EDGE_LANES * (i + 1))
            for k, start in enumerate((0, 30)):
                sums[k] = jnp.where(here, pltpu.roll(tile, (EDGE_LANES * i - start) % LANES, 1), sums[k])
            for k, ref in enumerate((o_ref, e_ref)):
                for s in range(3):
                    ref[3 * j + s] = r_ref[pl.ds(BLOCK * j + (0, 28)[k] + 8 * s, 8), :]
        o_ref[48 + g] = sums[0]
        e_ref[48 + g] = sums[1]


def side_beams(ref, steer_ref, halo_ref, side_ref):
    lane = lax.broadcasted_iota(jnp.int32, (8, LANES), 1)
    for j in range(16):
        tile = pltpu.roll(ref[48 + j // MERGED], -EDGE_LANES * (j % MERGED) % LANES, 1)
        halo_ref[j] = jnp.where(lane < EDGE_LANES, tile, 0.0)
    lines = ref[:48].reshape(16, 3, 8, LANES)
    for s in (0, 2):
        both = beam_pair(lines[:, s], lines[:, 1] if s == 0 else halo_ref[...], steer_ref)
        side_ref[s] = both[:, :LANES]
        side_ref[s + 1] = both[:, LANES:]


def beam_pair(first, second, steer_ref):
    both = jnp.concatenate([first.reshape(LANES, LANES), second.reshape(LANES, LANES)], axis=1)
    high = both.astype(jnp.bfloat16)
    low = (both - high.astype(jnp.float32)).astype(jnp.bfloat16)
    stacked = jnp.concatenate([high, low, high], axis=0)
    beams = jnp.dot(steer_ref[...], stacked, preferred_element_type=jnp.float32)
    beams = beams.reshape(HEIGHTS // 8, 2, 8, 2 * LANES)
    power = beams[:, 0] * beams[:, 0] + beams[:, 1] * beams[:, 1]
    squares = (both * both).reshape(16, 8, 2 * LANES).sum(axis=0)
    return jnp.concatenate([power.reshape(HEIGHTS, 2 * LANES), squares], axis=0)


def own_kernel(r_ref, halo_ref, steer_ref, out_ref):
    def block(s):
        if s == HALO:
            return halo_ref[...]
        (m,) = [m for m in SLOT if SLOT[m] == s]
        return jnp.concatenate([r_ref[pl.ds(BLOCK * j + ROW[m], 8), :] for j in range(16)], axis=0)

    for s in (0, 2, 4, 6, 8):
        t = min(s + 1, 8)
        both = beam_pair(block(s), block(t), steer_ref)
        out_ref[s] = both[:, :LANES]
        if t != s:
            out_ref[t] = both[:, LANES:]


def halves(field):
    high = field.astype(jnp.bfloat16)
    low = (field - high.astype(jnp.float32)).astype(jnp.bfloat16)
    return jnp.concatenate([high, low], axis=1)


def normalized(total, correction, band_ref):
    box = jnp.dot(halves(total), band_ref[...], preferred_element_type=jnp.float32) + correction
    energy = box[HEIGHTS:].sum(axis=0, keepdims=True)
    return box[:HEIGHTS] * (1.0 / (energy + epsilon))


def boxed(total, correction):
    lane = lax.broadcasted_iota(jnp.int32, total.shape, 1)

    def after(field, d):
        return jnp.where(lane >= d, pltpu.roll(field, d, 1), 0.0)

    def before(field, d):
        return jnp.where(lane < LANES - d, pltpu.roll(field, LANES - d, 1), 0.0)

    right, left = total + after(total, 1), before(total, 1)
    return (right + after(right, 2)) + (left + before(total + left, 2)) + correction


def normalize(box_of, ref):
    inverse = [1.0 / (box.sum(axis=0, keepdims=True) + epsilon) for box in box_of(slice(HEIGHTS, ROWS))]
    for k in range(0, HEIGHTS, 8):
        for n, box in enumerate(box_of(slice(k, k + 8))):
            ref[n, k : k + 8] = box * inverse[n]


def inner_kernel(own_ref, e_ref, steer_ref, mid_ref, me_ref, band_ref, done_ref, part_ref, cor_ref, halo_ref, side_ref, all_ref):
    side_beams(e_ref, steer_ref, halo_ref, side_ref)
    all_ref[...] = jnp.dot(halves(own_ref[HALO]), mid_ref[...], preferred_element_type=jnp.float32)
    all_ref[:, 5 * LANES :] += jnp.dot(halves(side_ref[3]), me_ref[...], preferred_element_type=jnp.float32)
    cor_ref[...] = all_ref[:, : 3 * LANES]

    def summed(m):
        total = None
        for position in range(max(m - 3, 0), m + 4):
            term = side_ref[position - 8] if position > 7 else own_ref[SLOT[position]]
            total = term if total is None else total + term
        return total

    for m in range(3, 8):
        done_ref[m - 3] = normalized(summed(m), all_ref[:, m * LANES : (m + 1) * LANES], band_ref)
    for m in range(3):
        part_ref[m] = summed(m)


def outer_kernel(o_ref, part_ref, cor_ref, lines_ref, steer_ref, mo_ref, out_ref, halo_ref, side_ref, all_ref, edge_ref, done_ref, sems):
    side_beams(o_ref, steer_ref, halo_ref, side_ref)
    all_ref[...] = cor_ref[...] + jnp.dot(halves(side_ref[3]), mo_ref[...], preferred_element_type=jnp.float32)

    def box_of(rows):
        near, next_, far = (side_ref[n, rows] for n in range(3))
        two = near + next_
        sums = (part_ref[0, rows] + (two + far), part_ref[1, rows] + two, part_ref[2, rows] + near)
        return [boxed(total, all_ref[rows, n * LANES : (n + 1) * LANES]) for n, total in enumerate(sums)]

    normalize(box_of, edge_ref)
    odd = parity() == 1
    copies = []
    for q in range(4):
        for k in range(64 * q, 64 * q + 64, 8):
            tiles = [edge_ref[m, k : k + 8] for m in range(3)] + [lines_ref[m, k : k + 8] for m in range(5)]
            done_ref[k : k + 8] = jnp.stack(transposed(turned(tiles, odd))).astype(jnp.bfloat16)
        copy = pltpu.make_async_copy(done_ref.at[pl.ds(64 * q, 64)], out_ref.at[pl.ds(64 * q, 64)], sems.at[q])
        copy.start()
        copies.append(copy)
    for copy in copies:
        copy.wait()


def spread():
    column = np.array([-3, -2, -1, 128, 129, 130])
    near = np.abs(column[:, None] - np.arange(LANES)[None, :]) <= 3

    def matrix(position_of, lines, used, first=0):
        full = np.zeros((LANES, len(lines), LANES), np.float32)
        for n in used:
            for i, m in enumerate(lines):
                if abs(position_of(n) - m) <= 3:
                    full[6 * (n - first) : 6 * (n - first) + 6, i] = near
        full = full.reshape(LANES, -1)
        return jnp.asarray(np.concatenate([full, full], axis=0), jnp.bfloat16)

    mid = matrix(lambda n: n, range(8), range(8))
    mo = matrix(lambda n: -1 - n, (0, 1, 2), (0, 1, 2))
    me = matrix(lambda n: 15 - n, (5, 6, 7), (5, 6, 7), 5)
    cell = np.arange(LANES)
    band = np.abs(cell[:, None] - cell[None, :]) <= 3
    return mid, mo, me, jnp.asarray(np.concatenate([band, band], axis=0), jnp.bfloat16)


def steering(wavenumbers):
    source = np.array([4 * acq + k for acq in PLACE for _ in range(2) for k in range(4)])
    chosen = np.arange(len(source) // 2)[:, None] == source[None, :]
    waves = jnp.sum(jnp.where(chosen, wavenumbers[:, None], 0.0), axis=0)
    real = (np.arange(LANES) // 4) % 2 == 0
    heights = np.arange(HEIGHTS, dtype=np.float32) - np.float32(HEIGHTS // 2)
    phases = jnp.asarray(heights)[:, None] * waves[None, :]
    cosine, sine = jnp.cos(phases), jnp.sin(phases)
    full = jnp.concatenate([jnp.where(real, cosine, sine), jnp.where(real, -sine, cosine)], axis=0)
    full = full.reshape(2, HEIGHTS // 8, 8, LANES).transpose(1, 0, 2, 3).reshape(2 * HEIGHTS, LANES)
    high = lax.reduce_precision(full, 8, 7)
    low = (full - high).astype(jnp.bfloat16)
    high = high.astype(jnp.bfloat16)
    return jnp.concatenate([high, high, low], axis=1)


VMEM = pl.BlockSpec(memory_space=pltpu.VMEM)
ANY = pl.BlockSpec(memory_space=pl.ANY)


def call(kernel, shapes, vmem, flops, scratch=(), out=VMEM, dtype=jnp.float32):
    def on(*operands):
        return pl.pallas_call(
            kernel,
            out_shape=[jax.ShapeDtypeStruct(shape, dtype) for shape in shapes],
            in_specs=[VMEM] * len(operands),
            out_specs=[out] * len(shapes),
            scratch_shapes=list(scratch),
            compiler_params=pltpu.CompilerParams(vmem_limit_bytes=vmem << 20),
            cost_estimate=pl.CostEstimate(flops=flops, bytes_accessed=1000000, transcendentals=0),
        )(*operands)

    return on


def spectrum(slc_stack, wavenumbers):
    lines = lax.axis_size("line")
    outer = [pair for i in range(1, lines - 1, 2) for pair in ((i, i + 1), (i + 1, i))]
    inner = [pair for i in range(0, lines, 2) for pair in ((i, i + 1), (i + 1, i))]
    strip = pltpu.VMEM((16, 8, LANES), jnp.float32)
    quad = pltpu.VMEM((4, ROWS, LANES), jnp.float32)
    stack = slc_stack.reshape(8, 8, -1, LANES).transpose(0, 2, 1, 3).reshape(-1, LANES)
    (packed,) = call(pack_kernel, [(16 * BLOCK, LANES)], 2, 1000000)(stack)
    packed = packed.reshape(16, BLOCK, 1, LANES)
    gathered = lax.all_to_all(packed, "acq", 0, 0, tiled=True, axis_index_groups=[PLACE])
    gathered = gathered.reshape(16 * BLOCK, LANES)
    sides = (EDGE_TILES, 8, LANES)
    to_o, to_e, halo = call(edge_kernel, [sides, sides, (16, 8, LANES)], 4, 1000000)(gathered)
    mid, mo, me, band = spread()
    to_o, to_e, wavenumbers = lax.optimization_barrier((to_o, to_e, wavenumbers))
    steer = steering(wavenumbers)
    side_o = lax.ppermute(to_o, "line", outer)
    side_e = lax.ppermute(to_e, "line", inner)
    (own,) = call(own_kernel, [(9, ROWS, LANES)], 10, 1000000000)(gathered, halo, steer)
    rest, part, cor = call(
        inner_kernel,
        [(5, HEIGHTS, LANES), (3, ROWS, LANES), (ROWS, 3 * LANES)],
        14,
        1000000000,
        [strip, quad, pltpu.VMEM((ROWS, 8 * LANES), jnp.float32)],
    )(own, side_e, steer, mid, me, band)
    (result,) = call(
        outer_kernel,
        [(HEIGHTS, 8, LANES)],
        12,
        1000000000,
        [
            strip,
            quad,
            pltpu.VMEM((ROWS, 3 * LANES), jnp.float32),
            pltpu.VMEM((3, HEIGHTS, LANES), jnp.float32),
            pltpu.VMEM((HEIGHTS, 8, LANES), jnp.bfloat16),
            pltpu.SemaphoreType.DMA((4,)),
        ],
        out=ANY,
        dtype=jnp.bfloat16,
    )(side_o, part, cor, rest, steer, mo)
    return result


def solution(mesh):
    placed = (P(None, "acq", "line", None), P())
    return jax.shard_map(spectrum, mesh=mesh, in_specs=placed, out_specs=P(None, "line", "acq"), check_vma=False)
```

```python
import jax
import jax.numpy as jnp
import numpy as np
from jax import lax
from jax.experimental import pallas as pl
from jax.experimental.pallas import tpu as pltpu
from jax.sharding import PartitionSpec as P


HEIGHTS = 256
ROWS = HEIGHTS + 8
LANES = 128
epsilon = 1e-06

ROW = {0: 0, 1: 8, 2: 16, 7: 28, 6: 36, 5: 44, 3: 52, 4: 60}
HALO_ROW = 24
BLOCK = 68
HELD = (26, 17)
SLOT = {0: 0, 1: 1, 2: 2, 7: 4, 6: 5, 5: 6, 3: 7, 4: 8}
HALO = 3
EDGE_LANES = 18
MERGED = 7
EDGE_TILES = 48 + 3
PLACE = [2 * z + y for z in (4, 3, 5, 2, 6, 1, 7, 0) for y in (0, 1)]


def parity():
    return lax.rem(lax.axis_index("line"), 2)


def transposed(tiles):
    sub = lax.broadcasted_iota(jnp.int32, (8, LANES), 0)
    tiles = list(tiles)
    for d in (4, 2, 1):
        low = (sub & d) == 0
        for i in range(8):
            if i & d == 0:
                a, b = tiles[i], tiles[i + d]
                tiles[i] = jnp.where(low, a, pltpu.roll(b, d, 0))
                tiles[i + d] = jnp.where(low, pltpu.roll(a, 8 - d, 0), b)
    return tiles


def turned(tiles, odd):
    return [jnp.where(odd, tiles[-1 - i], tile) for i, tile in enumerate(tiles)]


def pack(x_ref, out_ref):
    blocks = x_ref.shape[0] // 64
    odd = parity() == 1
    lane = lax.broadcasted_iota(jnp.int32, (8, LANES), 1)
    zero = jnp.zeros((8, LANES), jnp.float32)
    halo = [zero, zero]
    for j in range(blocks):
        halo.append(zero)
        rows = [slice(8 * (blocks * channel + j), 8 * (blocks * channel + j) + 8) for channel in range(8)]
        for m, tile in enumerate(turned(transposed([x_ref[r] for r in rows]), odd)):
            out_ref[pl.ds(BLOCK * PLACE.index(j) + ROW[m], 8), :] = tile
            left = (lane >= 6 * m) & (lane < 6 * m + 3)
            right = (lane >= 6 * m + 3) & (lane < 6 * m + 6)
            moved = pltpu.roll(tile, 6 * m + 3, 1)
            halo[j + 2] = jnp.where(left, moved, halo[j + 2])
            halo[j] = jnp.where(right, moved, halo[j])
    for j in range(blocks):
        tile = halo[j + 1]
        tile = tile + pltpu.roll(pltpu.roll(tile, 4, 0), LANES // 2, 1)
        out_ref[pl.ds(BLOCK * PLACE.index(j) + HALO_ROW, 4), :] = tile[:4]


def pack_kernel(x_ref, out_ref):
    line, lines = lax.axis_index("line"), lax.axis_size("line")
    row = lax.rem(line, 8)
    first, last = (row == 1) & (line > 1), (row == 6) & (line < lines - 2)
    times = 1 + jnp.where(first, HELD[0], jnp.where(last, HELD[1], 0))

    def once(_, carry):
        pack(x_ref, out_ref)
        return carry

    lax.fori_loop(0, times, once, 0)


def edge_kernel(r_ref, o_ref, e_ref, halo_ref):
    lane = lax.broadcasted_iota(jnp.int32, (8, LANES), 1)
    sub = lax.broadcasted_iota(jnp.int32, (8, LANES), 0)
    for g in range(3):
        sums = [jnp.zeros((8, LANES), jnp.float32) for _ in range(2)]
        for i in range(min(MERGED, 16 - MERGED * g)):
            j = MERGED * g + i
            tile = r_ref[pl.ds(BLOCK * j + HALO_ROW, 8), :]
            tile = jnp.where(sub < 4, tile, pltpu.roll(pltpu.roll(tile, 4, 0), LANES // 2, 1))
            tile = jnp.where(lane < 48, tile, 0.0)
            halo_ref[j] = tile
            here = (lane >= EDGE_LANES * i) & (lane < EDGE_LANES * (i + 1))
            for k, start in enumerate((0, 30)):
                sums[k] = jnp.where(here, pltpu.roll(tile, (EDGE_LANES * i - start) % LANES, 1), sums[k])
            for k, ref in enumerate((o_ref, e_ref)):
                for s in range(3):
                    ref[3 * j + s] = r_ref[pl.ds(BLOCK * j + (0, 28)[k] + 8 * s, 8), :]
        o_ref[48 + g] = sums[0]
        e_ref[48 + g] = sums[1]


def side_beams(ref, steer_ref, halo_ref, side_ref):
    lane = lax.broadcasted_iota(jnp.int32, (8, LANES), 1)
    for j in range(16):
        tile = pltpu.roll(ref[48 + j // MERGED], -EDGE_LANES * (j % MERGED) % LANES, 1)
        halo_ref[j] = jnp.where(lane < EDGE_LANES, tile, 0.0)
    lines = ref[:48].reshape(16, 3, 8, LANES)
    for s in (0, 2):
        both = beam_pair(lines[:, s], lines[:, 1] if s == 0 else halo_ref[...], steer_ref)
        side_ref[s] = both[:, :LANES]
        side_ref[s + 1] = both[:, LANES:]


def beam_pair(first, second, steer_ref):
    both = jnp.concatenate([first.reshape(LANES, LANES), second.reshape(LANES, LANES)], axis=1)
    high = both.astype(jnp.bfloat16)
    low = (both - high.astype(jnp.float32)).astype(jnp.bfloat16)
    stacked = jnp.concatenate([high, low, high], axis=0)
    beams = jnp.dot(steer_ref[...], stacked, preferred_element_type=jnp.float32)
    beams = beams.reshape(HEIGHTS // 8, 2, 8, 2 * LANES)
    power = beams[:, 0] * beams[:, 0] + beams[:, 1] * beams[:, 1]
    squares = (both * both).reshape(16, 8, 2 * LANES).sum(axis=0)
    return jnp.concatenate([power.reshape(HEIGHTS, 2 * LANES), squares], axis=0)


def own_kernel(r_ref, halo_ref, steer_ref, out_ref):
    def block(s):
        if s == HALO:
            return halo_ref[...]
        (m,) = [m for m in SLOT if SLOT[m] == s]
        return jnp.concatenate([r_ref[pl.ds(BLOCK * j + ROW[m], 8), :] for j in range(16)], axis=0)

    for s in (0, 2, 4, 6, 8):
        t = min(s + 1, 8)
        both = beam_pair(block(s), block(t), steer_ref)
        out_ref[s] = both[:, :LANES]
        if t != s:
            out_ref[t] = both[:, LANES:]


def halves(field):
    high = field.astype(jnp.bfloat16)
    low = (field - high.astype(jnp.float32)).astype(jnp.bfloat16)
    return jnp.concatenate([high, low], axis=1)


def normalized(total, correction, band_ref):
    box = jnp.dot(halves(total), band_ref[...], preferred_element_type=jnp.float32) + correction
    energy = box[HEIGHTS:].sum(axis=0, keepdims=True)
    return box[:HEIGHTS] * (1.0 / (energy + epsilon))


def boxed(total, correction):
    lane = lax.broadcasted_iota(jnp.int32, total.shape, 1)

    def after(field, d):
        return jnp.where(lane >= d, pltpu.roll(field, d, 1), 0.0)

    def before(field, d):
        return jnp.where(lane < LANES - d, pltpu.roll(field, LANES - d, 1), 0.0)

    right, left = total + after(total, 1), before(total, 1)
    return (right + after(right, 2)) + (left + before(total + left, 2)) + correction


def normalize(box_of, ref):
    inverse = [1.0 / (box.sum(axis=0, keepdims=True) + epsilon) for box in box_of(slice(HEIGHTS, ROWS))]
    for k in range(0, HEIGHTS, 8):
        for n, box in enumerate(box_of(slice(k, k + 8))):
            ref[n, k : k + 8] = box * inverse[n]


def inner_kernel(own_ref, e_ref, steer_ref, mid_ref, me_ref, band_ref, done_ref, part_ref, cor_ref, halo_ref, side_ref, all_ref):
    side_beams(e_ref, steer_ref, halo_ref, side_ref)
    all_ref[...] = jnp.dot(halves(own_ref[HALO]), mid_ref[...], preferred_element_type=jnp.float32)
    all_ref[:, 5 * LANES :] += jnp.dot(halves(side_ref[3]), me_ref[...], preferred_element_type=jnp.float32)
    cor_ref[...] = all_ref[:, : 3 * LANES]

    def summed(m):
        total = None
        for position in range(max(m - 3, 0), m + 4):
            term = side_ref[position - 8] if position > 7 else own_ref[SLOT[position]]
            total = term if total is None else total + term
        return total

    for m in range(3, 8):
        done_ref[m - 3] = normalized(summed(m), all_ref[:, m * LANES : (m + 1) * LANES], band_ref)
    for m in range(3):
        part_ref[m] = summed(m)


def outer_kernel(o_ref, part_ref, cor_ref, lines_ref, steer_ref, mo_ref, out_ref, halo_ref, side_ref, all_ref, edge_ref, done_ref, sems):
    side_beams(o_ref, steer_ref, halo_ref, side_ref)
    all_ref[...] = cor_ref[...] + jnp.dot(halves(side_ref[3]), mo_ref[...], preferred_element_type=jnp.float32)

    def box_of(rows):
        near, next_, far = (side_ref[n, rows] for n in range(3))
        two = near + next_
        sums = (part_ref[0, rows] + (two + far), part_ref[1, rows] + two, part_ref[2, rows] + near)
        return [boxed(total, all_ref[rows, n * LANES : (n + 1) * LANES]) for n, total in enumerate(sums)]

    normalize(box_of, edge_ref)
    odd = parity() == 1
    copies = []
    for q in range(4):
        for k in range(64 * q, 64 * q + 64, 8):
            tiles = [edge_ref[m, k : k + 8] for m in range(3)] + [lines_ref[m, k : k + 8] for m in range(5)]
            done_ref[k : k + 8] = jnp.stack(transposed(turned(tiles, odd))).astype(jnp.bfloat16)
        copy = pltpu.make_async_copy(done_ref.at[pl.ds(64 * q, 64)], out_ref.at[pl.ds(64 * q, 64)], sems.at[q])
        copy.start()
        copies.append(copy)
    for copy in copies:
        copy.wait()


def copy_kernel(x_ref, out_ref):
    out_ref[...] = x_ref[...]


def spread():
    column = np.array([-3, -2, -1, 128, 129, 130])
    near = np.abs(column[:, None] - np.arange(LANES)[None, :]) <= 3

    def matrix(position_of, lines, used, first=0):
        full = np.zeros((LANES, len(lines), LANES), np.float32)
        for n in used:
            for i, m in enumerate(lines):
                if abs(position_of(n) - m) <= 3:
                    full[6 * (n - first) : 6 * (n - first) + 6, i] = near
        full = full.reshape(LANES, -1)
        return jnp.asarray(np.concatenate([full, full], axis=0), jnp.bfloat16)

    mid = matrix(lambda n: n, range(8), range(8))
    mo = matrix(lambda n: -1 - n, (0, 1, 2), (0, 1, 2))
    me = matrix(lambda n: 15 - n, (5, 6, 7), (5, 6, 7), 5)
    cell = np.arange(LANES)
    band = np.abs(cell[:, None] - cell[None, :]) <= 3
    return mid, mo, me, jnp.asarray(np.concatenate([band, band], axis=0), jnp.bfloat16)


def steering(wavenumbers):
    source = np.array([4 * acq + k for acq in PLACE for _ in range(2) for k in range(4)])
    chosen = np.arange(len(source) // 2)[:, None] == source[None, :]
    waves = jnp.sum(jnp.where(chosen, wavenumbers[:, None], 0.0), axis=0)
    real = (np.arange(LANES) // 4) % 2 == 0
    heights = np.arange(HEIGHTS, dtype=np.float32) - np.float32(HEIGHTS // 2)
    phases = jnp.asarray(heights)[:, None] * waves[None, :]
    cosine, sine = jnp.cos(phases), jnp.sin(phases)
    full = jnp.concatenate([jnp.where(real, cosine, sine), jnp.where(real, -sine, cosine)], axis=0)
    full = full.reshape(2, HEIGHTS // 8, 8, LANES).transpose(1, 0, 2, 3).reshape(2 * HEIGHTS, LANES)
    high = lax.reduce_precision(full, 8, 7)
    low = (full - high).astype(jnp.bfloat16)
    high = high.astype(jnp.bfloat16)
    return jnp.concatenate([high, high, low], axis=1)


VMEM = pl.BlockSpec(memory_space=pltpu.VMEM)
ANY = pl.BlockSpec(memory_space=pl.ANY)


def call(kernel, shapes, vmem, flops, scratch=(), out=VMEM, dtype=jnp.float32):
    def on(*operands):
        return pl.pallas_call(
            kernel,
            out_shape=[jax.ShapeDtypeStruct(shape, dtype) for shape in shapes],
            in_specs=[VMEM] * len(operands),
            out_specs=[out] * len(shapes),
            scratch_shapes=list(scratch),
            compiler_params=pltpu.CompilerParams(vmem_limit_bytes=vmem << 20),
            cost_estimate=pl.CostEstimate(flops=flops, bytes_accessed=1000000, transcendentals=0),
        )(*operands)

    return on


def spectrum(slc_stack, wavenumbers):
    lines = lax.axis_size("line")
    outer = [pair for i in range(1, lines - 1, 2) for pair in ((i, i + 1), (i + 1, i))]
    inner = [pair for i in range(0, lines, 2) for pair in ((i, i + 1), (i + 1, i))]
    strip = pltpu.VMEM((16, 8, LANES), jnp.float32)
    quad = pltpu.VMEM((4, ROWS, LANES), jnp.float32)
    stack = slc_stack.reshape(8, 8, -1, LANES).transpose(0, 2, 1, 3).reshape(-1, LANES)
    (packed,) = call(pack_kernel, [(16 * BLOCK, LANES)], 2, 1000000)(stack)
    packed = packed.reshape(16, BLOCK, 1, LANES)
    gathered = lax.all_to_all(packed, "acq", 0, 0, tiled=True, axis_index_groups=[PLACE])
    gathered = gathered.reshape(16 * BLOCK, LANES)
    sides = (EDGE_TILES, 8, LANES)
    to_o, to_e, halo = call(edge_kernel, [sides, sides, (16, 8, LANES)], 4, 1000000)(gathered)
    mid, mo, me, band = spread()
    to_o, to_e, wavenumbers = lax.optimization_barrier((to_o, to_e, wavenumbers))
    (wavenumbers,) = call(copy_kernel, [(1, wavenumbers.shape[0])], 1, 1000)(wavenumbers.reshape(1, -1))
    steer = steering(wavenumbers.reshape(-1))
    side_o = lax.ppermute(to_o, "line", outer)
    side_e = lax.ppermute(to_e, "line", inner)
    (own,) = call(own_kernel, [(9, ROWS, LANES)], 10, 1000000000)(gathered, halo, steer)
    rest, part, cor = call(
        inner_kernel,
        [(5, HEIGHTS, LANES), (3, ROWS, LANES), (ROWS, 3 * LANES)],
        14,
        1000000000,
        [strip, quad, pltpu.VMEM((ROWS, 8 * LANES), jnp.float32)],
    )(own, side_e, steer, mid, me, band)
    (result,) = call(
        outer_kernel,
        [(HEIGHTS, 8, LANES)],
        12,
        1000000000,
        [
            strip,
            quad,
            pltpu.VMEM((ROWS, 3 * LANES), jnp.float32),
            pltpu.VMEM((3, HEIGHTS, LANES), jnp.float32),
            pltpu.VMEM((HEIGHTS, 8, LANES), jnp.bfloat16),
            pltpu.SemaphoreType.DMA((4,)),
        ],
        out=ANY,
        dtype=jnp.bfloat16,
    )(side_o, part, cor, rest, steer, mo)
    return result


def solution(mesh):
    placed = (P(None, "acq", "line", None), P())
    return jax.shard_map(spectrum, mesh=mesh, in_specs=placed, out_specs=P(None, "line", "acq"), check_vma=False)
```

```python
import jax
import jax.numpy as jnp
import numpy as np
from jax import lax
from jax.experimental import pallas as pl
from jax.experimental.pallas import tpu as pltpu
from jax.sharding import PartitionSpec as P


HEIGHTS = 256
ROWS = HEIGHTS + 8
LANES = 128
epsilon = 1e-06

ROW = {0: 0, 1: 8, 2: 16, 7: 28, 6: 36, 5: 44, 3: 52, 4: 60}
HALO_ROW = 24
BLOCK = 68
HELD = (26, 17)
SLOT = {0: 0, 1: 1, 2: 2, 7: 4, 6: 5, 5: 6, 3: 7, 4: 8}
HALO = 3
EDGE_LANES = 18
MERGED = 7
EDGE_TILES = 48 + 3
PLACE = [2 * z + y for z in (4, 3, 5, 2, 6, 1, 7, 0) for y in (0, 1)]


def parity():
    return lax.rem(lax.axis_index("line"), 2)


def transposed(tiles):
    sub = lax.broadcasted_iota(jnp.int32, (8, LANES), 0)
    tiles = list(tiles)
    for d in (4, 2, 1):
        low = (sub & d) == 0
        for i in range(8):
            if i & d == 0:
                a, b = tiles[i], tiles[i + d]
                tiles[i] = jnp.where(low, a, pltpu.roll(b, d, 0))
                tiles[i + d] = jnp.where(low, pltpu.roll(a, 8 - d, 0), b)
    return tiles


def turned(tiles, odd):
    return [jnp.where(odd, tiles[-1 - i], tile) for i, tile in enumerate(tiles)]


def pack(x_ref, out_ref):
    blocks = x_ref.shape[0] // 64
    odd = parity() == 1
    lane = lax.broadcasted_iota(jnp.int32, (8, LANES), 1)
    zero = jnp.zeros((8, LANES), jnp.float32)
    halo = [zero, zero]
    for j in range(blocks):
        halo.append(zero)
        rows = [slice(8 * (blocks * channel + j), 8 * (blocks * channel + j) + 8) for channel in range(8)]
        for m, tile in enumerate(turned(transposed([x_ref[r] for r in rows]), odd)):
            out_ref[pl.ds(BLOCK * PLACE.index(j) + ROW[m], 8), :] = tile
            left = (lane >= 6 * m) & (lane < 6 * m + 3)
            right = (lane >= 6 * m + 3) & (lane < 6 * m + 6)
            moved = pltpu.roll(tile, 6 * m + 3, 1)
            halo[j + 2] = jnp.where(left, moved, halo[j + 2])
            halo[j] = jnp.where(right, moved, halo[j])
    for j in range(blocks):
        tile = halo[j + 1]
        tile = tile + pltpu.roll(pltpu.roll(tile, 4, 0), LANES // 2, 1)
        out_ref[pl.ds(BLOCK * PLACE.index(j) + HALO_ROW, 4), :] = tile[:4]


def pack_kernel(x_ref, out_ref):
    line, lines = lax.axis_index("line"), lax.axis_size("line")
    row = lax.rem(line, 8)
    first, last = (row == 1) & (line > 1), (row == 6) & (line < lines - 2)
    times = 1 + jnp.where(first, HELD[0], jnp.where(last, HELD[1], 0))

    def once(_, carry):
        pack(x_ref, out_ref)
        return carry

    lax.fori_loop(0, times, once, 0)


def edge_kernel(r_ref, o_ref, e_ref, halo_ref):
    lane = lax.broadcasted_iota(jnp.int32, (8, LANES), 1)
    sub = lax.broadcasted_iota(jnp.int32, (8, LANES), 0)
    for g in range(3):
        sums = [jnp.zeros((8, LANES), jnp.float32) for _ in range(2)]
        for i in range(min(MERGED, 16 - MERGED * g)):
            j = MERGED * g + i
            tile = r_ref[pl.ds(BLOCK * j + HALO_ROW, 8), :]
            tile = jnp.where(sub < 4, tile, pltpu.roll(pltpu.roll(tile, 4, 0), LANES // 2, 1))
            tile = jnp.where(lane < 48, tile, 0.0)
            halo_ref[j] = tile
            here = (lane >= EDGE_LANES * i) & (lane < EDGE_LANES * (i + 1))
            for k, start in enumerate((0, 30)):
                sums[k] = jnp.where(here, pltpu.roll(tile, (EDGE_LANES * i - start) % LANES, 1), sums[k])
            for k, ref in enumerate((o_ref, e_ref)):
                for s in range(3):
                    ref[3 * j + s] = r_ref[pl.ds(BLOCK * j + (0, 28)[k] + 8 * s, 8), :]
        o_ref[48 + g] = sums[0]
        e_ref[48 + g] = sums[1]


def side_beams(ref, steer_ref, halo_ref, side_ref):
    lane = lax.broadcasted_iota(jnp.int32, (8, LANES), 1)
    for j in range(16):
        tile = pltpu.roll(ref[48 + j // MERGED], -EDGE_LANES * (j % MERGED) % LANES, 1)
        halo_ref[j] = jnp.where(lane < EDGE_LANES, tile, 0.0)
    lines = ref[:48].reshape(16, 3, 8, LANES)
    for s in (0, 2):
        both = beam_pair(lines[:, s], lines[:, 1] if s == 0 else halo_ref[...], steer_ref)
        side_ref[s] = both[:, :LANES]
        side_ref[s + 1] = both[:, LANES:]


def beam_pair(first, second, steer_ref):
    both = jnp.concatenate([first.reshape(LANES, LANES), second.reshape(LANES, LANES)], axis=1)
    high = both.astype(jnp.bfloat16)
    low = (both - high.astype(jnp.float32)).astype(jnp.bfloat16)
    stacked = jnp.concatenate([high, low, high], axis=0)
    beams = jnp.dot(steer_ref[...], stacked, preferred_element_type=jnp.float32)
    beams = beams.reshape(HEIGHTS // 8, 2, 8, 2 * LANES)
    power = beams[:, 0] * beams[:, 0] + beams[:, 1] * beams[:, 1]
    squares = (both * both).reshape(16, 8, 2 * LANES).sum(axis=0)
    return jnp.concatenate([power.reshape(HEIGHTS, 2 * LANES), squares], axis=0)


def own_kernel(r_ref, halo_ref, steer_ref, out_ref):
    def block(s):
        if s == HALO:
            return halo_ref[...]
        (m,) = [m for m in SLOT if SLOT[m] == s]
        return jnp.concatenate([r_ref[pl.ds(BLOCK * j + ROW[m], 8), :] for j in range(16)], axis=0)

    for s in (0, 2, 4, 6, 8):
        t = min(s + 1, 8)
        both = beam_pair(block(s), block(t), steer_ref)
        out_ref[s] = both[:, :LANES]
        if t != s:
            out_ref[t] = both[:, LANES:]


def halves(field):
    high = field.astype(jnp.bfloat16)
    low = (field - high.astype(jnp.float32)).astype(jnp.bfloat16)
    return jnp.concatenate([high, low], axis=1)


def normalized(total, correction, band_ref):
    box = jnp.dot(halves(total), band_ref[...], preferred_element_type=jnp.float32) + correction
    energy = box[HEIGHTS:].sum(axis=0, keepdims=True)
    return box[:HEIGHTS] * (1.0 / (energy + epsilon))


def boxed(total, correction):
    lane = lax.broadcasted_iota(jnp.int32, total.shape, 1)

    def after(field, d):
        return jnp.where(lane >= d, pltpu.roll(field, d, 1), 0.0)

    def before(field, d):
        return jnp.where(lane < LANES - d, pltpu.roll(field, LANES - d, 1), 0.0)

    right, left = total + after(total, 1), before(total, 1)
    return (right + after(right, 2)) + (left + before(total + left, 2)) + correction


def inner_kernel(own_ref, e_ref, steer_ref, mid_ref, me_ref, band_ref, done_ref, part_ref, cor_ref, halo_ref, side_ref, all_ref):
    side_beams(e_ref, steer_ref, halo_ref, side_ref)
    all_ref[...] = jnp.dot(halves(own_ref[HALO]), mid_ref[...], preferred_element_type=jnp.float32)
    all_ref[:, 5 * LANES :] += jnp.dot(halves(side_ref[3]), me_ref[...], preferred_element_type=jnp.float32)
    cor_ref[...] = all_ref[:, : 3 * LANES]

    def summed(m):
        total = None
        for position in range(max(m - 3, 0), m + 4):
            term = side_ref[position - 8] if position > 7 else own_ref[SLOT[position]]
            total = term if total is None else total + term
        return total

    for m in range(3, 8):
        done_ref[m - 3] = normalized(summed(m), all_ref[:, m * LANES : (m + 1) * LANES], band_ref)
    for m in range(3):
        part_ref[m] = summed(m)


def outer_kernel(o_ref, part_ref, cor_ref, lines_ref, steer_ref, mo_ref, out_ref, halo_ref, side_ref, all_ref, done_ref, sems):
    side_beams(o_ref, steer_ref, halo_ref, side_ref)
    all_ref[...] = cor_ref[...] + jnp.dot(halves(side_ref[3]), mo_ref[...], preferred_element_type=jnp.float32)

    def box_of(rows):
        near, next_, far = (side_ref[n, rows] for n in range(3))
        two = near + next_
        sums = (part_ref[0, rows] + (two + far), part_ref[1, rows] + two, part_ref[2, rows] + near)
        return [boxed(total, all_ref[rows, n * LANES : (n + 1) * LANES]) for n, total in enumerate(sums)]

    inverse = [1.0 / (box.sum(axis=0, keepdims=True) + epsilon) for box in box_of(slice(HEIGHTS, ROWS))]
    odd = parity() == 1
    copies = []
    for q in range(4):
        for k in range(64 * q, 64 * q + 64, 8):
            near = [box * scale for box, scale in zip(box_of(slice(k, k + 8)), inverse)]
            tiles = near + [lines_ref[m, k : k + 8] for m in range(5)]
            done_ref[k : k + 8] = jnp.stack(transposed(turned(tiles, odd))).astype(jnp.bfloat16)
        copy = pltpu.make_async_copy(done_ref.at[pl.ds(64 * q, 64)], out_ref.at[pl.ds(64 * q, 64)], sems.at[q])
        copy.start()
        copies.append(copy)
    for copy in copies:
        copy.wait()


def copy_kernel(x_ref, out_ref):
    out_ref[...] = x_ref[...]


def spread():
    column = np.array([-3, -2, -1, 128, 129, 130])
    near = np.abs(column[:, None] - np.arange(LANES)[None, :]) <= 3

    def matrix(position_of, lines, used, first=0):
        full = np.zeros((LANES, len(lines), LANES), np.float32)
        for n in used:
            for i, m in enumerate(lines):
                if abs(position_of(n) - m) <= 3:
                    full[6 * (n - first) : 6 * (n - first) + 6, i] = near
        full = full.reshape(LANES, -1)
        return jnp.asarray(np.concatenate([full, full], axis=0), jnp.bfloat16)

    mid = matrix(lambda n: n, range(8), range(8))
    mo = matrix(lambda n: -1 - n, (0, 1, 2), (0, 1, 2))
    me = matrix(lambda n: 15 - n, (5, 6, 7), (5, 6, 7), 5)
    cell = np.arange(LANES)
    band = np.abs(cell[:, None] - cell[None, :]) <= 3
    return mid, mo, me, jnp.asarray(np.concatenate([band, band], axis=0), jnp.bfloat16)


def steering(wavenumbers):
    source = np.array([4 * acq + k for acq in PLACE for _ in range(2) for k in range(4)])
    chosen = np.arange(len(source) // 2)[:, None] == source[None, :]
    waves = jnp.sum(jnp.where(chosen, wavenumbers[:, None], 0.0), axis=0)
    real = (np.arange(LANES) // 4) % 2 == 0
    heights = np.arange(HEIGHTS, dtype=np.float32) - np.float32(HEIGHTS // 2)
    phases = jnp.asarray(heights)[:, None] * waves[None, :]
    cosine, sine = jnp.cos(phases), jnp.sin(phases)
    full = jnp.concatenate([jnp.where(real, cosine, sine), jnp.where(real, -sine, cosine)], axis=0)
    full = full.reshape(2, HEIGHTS // 8, 8, LANES).transpose(1, 0, 2, 3).reshape(2 * HEIGHTS, LANES)
    high = lax.reduce_precision(full, 8, 7)
    low = (full - high).astype(jnp.bfloat16)
    high = high.astype(jnp.bfloat16)
    return jnp.concatenate([high, high, low], axis=1)


VMEM = pl.BlockSpec(memory_space=pltpu.VMEM)
ANY = pl.BlockSpec(memory_space=pl.ANY)


def call(kernel, shapes, vmem, flops, scratch=(), out=VMEM, dtype=jnp.float32):
    def on(*operands):
        return pl.pallas_call(
            kernel,
            out_shape=[jax.ShapeDtypeStruct(shape, dtype) for shape in shapes],
            in_specs=[VMEM] * len(operands),
            out_specs=[out] * len(shapes),
            scratch_shapes=list(scratch),
            compiler_params=pltpu.CompilerParams(vmem_limit_bytes=vmem << 20),
            cost_estimate=pl.CostEstimate(flops=flops, bytes_accessed=1000000, transcendentals=0),
        )(*operands)

    return on


def spectrum(slc_stack, wavenumbers):
    lines = lax.axis_size("line")
    outer = [pair for i in range(1, lines - 1, 2) for pair in ((i, i + 1), (i + 1, i))]
    inner = [pair for i in range(0, lines, 2) for pair in ((i, i + 1), (i + 1, i))]
    strip = pltpu.VMEM((16, 8, LANES), jnp.float32)
    quad = pltpu.VMEM((4, ROWS, LANES), jnp.float32)
    stack = slc_stack.reshape(8, 8, -1, LANES).transpose(0, 2, 1, 3).reshape(-1, LANES)
    (packed,) = call(pack_kernel, [(16 * BLOCK, LANES)], 2, 1000000)(stack)
    packed = packed.reshape(16, BLOCK, 1, LANES)
    gathered = lax.all_to_all(packed, "acq", 0, 0, tiled=True, axis_index_groups=[PLACE])
    gathered = gathered.reshape(16 * BLOCK, LANES)
    sides = (EDGE_TILES, 8, LANES)
    to_o, to_e, halo = call(edge_kernel, [sides, sides, (16, 8, LANES)], 4, 1000000)(gathered)
    mid, mo, me, band = spread()
    to_o, to_e, wavenumbers = lax.optimization_barrier((to_o, to_e, wavenumbers))
    (wavenumbers,) = call(copy_kernel, [(1, wavenumbers.shape[0])], 1, 1000)(wavenumbers.reshape(1, -1))
    steer = steering(wavenumbers.reshape(-1))
    side_o = lax.ppermute(to_o, "line", outer)
    side_e = lax.ppermute(to_e, "line", inner)
    (own,) = call(own_kernel, [(9, ROWS, LANES)], 10, 1000000000)(gathered, halo, steer)
    rest, part, cor = call(
        inner_kernel,
        [(5, HEIGHTS, LANES), (3, ROWS, LANES), (ROWS, 3 * LANES)],
        14,
        1000000000,
        [strip, quad, pltpu.VMEM((ROWS, 8 * LANES), jnp.float32)],
    )(own, side_e, steer, mid, me, band)
    (result,) = call(
        outer_kernel,
        [(HEIGHTS, 8, LANES)],
        12,
        1000000000,
        [
            strip,
            quad,
            pltpu.VMEM((ROWS, 3 * LANES), jnp.float32),
            pltpu.VMEM((HEIGHTS, 8, LANES), jnp.bfloat16),
            pltpu.SemaphoreType.DMA((4,)),
        ],
        out=ANY,
        dtype=jnp.bfloat16,
    )(side_o, part, cor, rest, steer, mo)
    return result


def solution(mesh):
    placed = (P(None, "acq", "line", None), P())
    return jax.shard_map(spectrum, mesh=mesh, in_specs=placed, out_specs=P(None, "line", "acq"), check_vma=False)
```
